32 devices in a mesh: pool: 32 (over z, y, x, core).
Axes of the slice: x: 2, y: 2, z: 4, core: 2. Of those that a mesh axis runs over, the one named last changes fastest.
Arguments:
- hidden: bfloat16 [32, 64, 7168], P('pool')
- prefix_len: int32 [32], P('pool')
- prefix_table: int32 [32, 64, 2], P('pool')
- write_table: int32 [32, 1, 2], P('pool')
- cache_c: bfloat16 [32, 65, 64, 512], P('pool')
- cache_kr: bfloat16 [32, 65, 64, 64], P('pool')
- w_q: bfloat16 [7168, 12288], replicated
- w_dkv: bfloat16 [7168, 576], replicated
- g_kv: bfloat16 [512], replicated
- w_uk: bfloat16 [512, 64, 128], replicated
- w_uv: bfloat16 [512, 64, 128], replicated
- w_o: bfloat16 [8192, 7168], replicated
Outputs:
- output 1: bfloat16 [32, 64, 7168], P('pool')
- output 2: bfloat16 [32, 65, 64, 512], P('pool')
- output 3: bfloat16 [32, 65, 64, 64], P('pool')
All inputs are finite; a program needn't handle non-finite values.
Results may differ from the reference program's by a relative error of at most 0.00640782.
Values are sent between devices in bfloat16 or wider.
A program may use at most 1.25 GiB of HBM per device.

```python
import math
import jax
import jax.numpy as jnp
from jax import lax

POOL_SIZE = 32
REQ_DEV = 1
CHUNK_LEN = 64
PREFIX_MAX = 4096
PREFIX_PAGES = 64
D_MODEL = 7168
NUM_HEADS = 64
PAGE_LEN = 64
LATENT = 512
ROPE_DIM = 64
NOPE_DIM = 128
VALUE_DIM = 128

REQUESTS = POOL_SIZE * REQ_DEV
TABLE_PAGES = PREFIX_MAX // PAGE_LEN
CHUNK_PAGES = CHUNK_LEN // PAGE_LEN
CACHE_PAGES = PREFIX_PAGES + REQ_DEV * CHUNK_PAGES
READ_SLOTS = max(1, (2 * REQ_DEV * TABLE_PAGES) // POOL_SIZE)
NORM_EPS = 1e-6
ROPE_BASE = 10000.0


def rope_tables(positions):
    half_dim = ROPE_DIM // 2
    inv_freq = ROPE_BASE ** (-jnp.arange(half_dim, dtype=jnp.float32) / half_dim)
    angles = positions.astype(jnp.float32)[..., None] * inv_freq
    return jnp.cos(angles), jnp.sin(angles)


def apply_rope(values, cos_tab, sin_tab):
    half_dim = ROPE_DIM // 2
    first = values[..., :half_dim]
    second = values[..., half_dim:]
    return jnp.concatenate([first * cos_tab - second * sin_tab, second * cos_tab + first * sin_tab], axis=-1)


def draw_tables(key):
    key_len, key_perm, key_rot, key_page, key_write = jax.random.split(key, 5)
    req_ids = jnp.arange(REQUESTS)
    page_counts = jax.random.randint(key_len, (REQUESTS,), 0, TABLE_PAGES + 1)
    page_counts = jnp.where(req_ids == 0, TABLE_PAGES, jnp.where(req_ids == REQUESTS - 1, 0, page_counts))
    prefix_len = (page_counts * PAGE_LEN).astype(jnp.int32)
    is_valid = (jnp.arange(TABLE_PAGES)[None, :] < page_counts[:, None]).reshape(POOL_SIZE, REQ_DEV * TABLE_PAGES)
    slot_rank = jnp.cumsum(is_valid.astype(jnp.int32), axis=1) - 1
    owner_perm = jax.random.permutation(key_perm, POOL_SIZE)
    rotation = jax.random.randint(key_rot, (POOL_SIZE, 1), 0, max(1, POOL_SIZE // 4))
    owners = owner_perm[(rotation + slot_rank // READ_SLOTS) % POOL_SIZE]
    page_pick = jax.random.randint(key_page, (POOL_SIZE, REQ_DEV * TABLE_PAGES), 0, PREFIX_PAGES)
    prefix_table = jnp.stack([jnp.where(is_valid, owners, -1), jnp.where(is_valid, page_pick, -1)], axis=-1)
    prefix_table = prefix_table.reshape(REQUESTS, TABLE_PAGES, 2).astype(jnp.int32)
    write_ids = jnp.arange(REQ_DEV * CHUNK_PAGES)
    offsets = jax.random.permutation(key_write, POOL_SIZE)[write_ids % POOL_SIZE]
    write_owner = (jnp.arange(POOL_SIZE)[:, None] + offsets[None, :]) % POOL_SIZE
    write_page = jnp.broadcast_to(PREFIX_PAGES + write_ids[None, :], (POOL_SIZE, REQ_DEV * CHUNK_PAGES))
    write_table = jnp.stack([write_owner, write_page], axis=-1).reshape(REQUESTS, CHUNK_PAGES, 2).astype(jnp.int32)
    return prefix_len, prefix_table, write_table


def setup_inputs(seed: int = 0) -> dict:
    key_list = jax.random.split(jax.random.key(seed), 12)
    prefix_len, prefix_table, write_table = draw_tables(key_list[0])
    q_gain = math.sqrt(math.log((PREFIX_MAX + CHUNK_LEN) / 8.0) / 3.0)
    hidden = jax.random.normal(key_list[1], (REQUESTS, CHUNK_LEN, D_MODEL), jnp.float32)
    cache_c = jax.random.normal(key_list[2], (POOL_SIZE, CACHE_PAGES, PAGE_LEN, LATENT), jnp.float32)
    cache_kr = jax.random.normal(key_list[3], (POOL_SIZE, CACHE_PAGES, PAGE_LEN, ROPE_DIM), jnp.float32)
    w_q = jax.random.normal(key_list[4], (D_MODEL, NUM_HEADS * (NOPE_DIM + ROPE_DIM)), jnp.float32) * (q_gain / math.sqrt(D_MODEL))
    w_dkv = jax.random.normal(key_list[5], (D_MODEL, LATENT + ROPE_DIM), jnp.float32) / math.sqrt(D_MODEL)
    g_kv = jax.random.uniform(key_list[6], (LATENT,), jnp.float32, 0.5, 1.5)
    w_uk = jax.random.normal(key_list[7], (LATENT, NUM_HEADS, NOPE_DIM), jnp.float32) / math.sqrt(NOPE_DIM)
    w_uv = jax.random.normal(key_list[8], (LATENT, NUM_HEADS, VALUE_DIM), jnp.float32) / math.sqrt(LATENT)
    w_o = jax.random.normal(key_list[9], (NUM_HEADS * VALUE_DIM, D_MODEL), jnp.float32) / math.sqrt(NUM_HEADS * VALUE_DIM)
    return {
        "hidden": hidden.astype(jnp.bfloat16),
        "prefix_len": prefix_len,
        "prefix_table": prefix_table,
        "write_table": write_table,
        "cache_c": cache_c.astype(jnp.bfloat16),
        "cache_kr": cache_kr.astype(jnp.bfloat16),
        "w_q": w_q.astype(jnp.bfloat16),
        "w_dkv": w_dkv.astype(jnp.bfloat16),
        "g_kv": g_kv.astype(jnp.bfloat16),
        "w_uk": w_uk.astype(jnp.bfloat16),
        "w_uv": w_uv.astype(jnp.bfloat16),
        "w_o": w_o.astype(jnp.bfloat16),
    }


def reference(hidden, prefix_len, prefix_table, write_table, cache_c, cache_kr, w_q, w_dkv, g_kv, w_uk, w_uv, w_o):
    flat_c = cache_c.reshape(POOL_SIZE * CACHE_PAGES, PAGE_LEN, LATENT)
    flat_kr = cache_kr.reshape(POOL_SIZE * CACHE_PAGES, PAGE_LEN, ROPE_DIM)
    score_scale = (NOPE_DIM + ROPE_DIM) ** -0.5
    w_uk32 = w_uk.astype(jnp.float32)
    w_uv32 = w_uv.astype(jnp.float32)
    kv_gain = g_kv.astype(jnp.float32)
    query_ids = jnp.arange(CHUNK_LEN)
    key_ids = jnp.arange(PREFIX_MAX + CHUNK_LEN)

    def one_request(req_item):
        x_req, pre_len, req_table = req_item
        page_ids = jnp.maximum(req_table[:, 0], 0) * CACHE_PAGES + jnp.maximum(req_table[:, 1], 0)
        pre_c = flat_c[page_ids].reshape(PREFIX_MAX, LATENT)
        pre_kr = flat_kr[page_ids].reshape(PREFIX_MAX, ROPE_DIM)
        q_all = jnp.dot(x_req, w_q, preferred_element_type=jnp.float32).astype(jnp.bfloat16)
        q_all = q_all.reshape(CHUNK_LEN, NUM_HEADS, NOPE_DIM + ROPE_DIM)
        kv_lat = jnp.dot(x_req, w_dkv, preferred_element_type=jnp.float32)
        lat_part = kv_lat[:, :LATENT]
        inv_rms = lax.rsqrt(jnp.mean(lat_part * lat_part, axis=-1, keepdims=True) + NORM_EPS)
        c_new = (lat_part * inv_rms * kv_gain).astype(jnp.bfloat16)
        cos_tab, sin_tab = rope_tables(pre_len + query_ids)
        kr_new = apply_rope(kv_lat[:, LATENT:], cos_tab, sin_tab).astype(jnp.bfloat16)
        q_rope = apply_rope(q_all[:, :, NOPE_DIM:].astype(jnp.float32), cos_tab[:, None, :], sin_tab[:, None, :]).astype(jnp.bfloat16)
        q_lat = jnp.einsum("chn,lhn->chl", q_all[:, :, :NOPE_DIM].astype(jnp.float32), w_uk32).astype(jnp.bfloat16)
        keys_c = jnp.concatenate([pre_c, c_new], axis=0).astype(jnp.float32)
        keys_r = jnp.concatenate([pre_kr, kr_new], axis=0).astype(jnp.float32)
        scores = jnp.einsum("chl,jl->hcj", q_lat.astype(jnp.float32), keys_c)
        scores = (scores + jnp.einsum("chr,jr->hcj", q_rope.astype(jnp.float32), keys_r)) * score_scale
        visible = jnp.where(key_ids[None, :] < PREFIX_MAX, key_ids[None, :] < pre_len, key_ids[None, :] - PREFIX_MAX <= query_ids[:, None])
        scores = jnp.where(visible[None, :, :], scores, -jnp.inf)
        weights = jax.nn.softmax(scores, axis=-1)
        o_lat = jnp.einsum("hcj,jl->chl", weights, keys_c).astype(jnp.bfloat16)
        o_heads = jnp.einsum("chl,lhv->chv", o_lat.astype(jnp.float32), w_uv32).astype(jnp.bfloat16)
        attn_out = jnp.dot(o_heads.reshape(CHUNK_LEN, NUM_HEADS * VALUE_DIM), w_o, preferred_element_type=jnp.float32)
        y_req = (x_req.astype(jnp.float32) + attn_out).astype(jnp.bfloat16)
        return y_req, c_new, kr_new

    hidden_out, new_c, new_kr = lax.map(one_request, (hidden, prefix_len, prefix_table))
    dest_rows = (write_table[:, :, 0] * CACHE_PAGES + write_table[:, :, 1]).reshape(REQUESTS * CHUNK_PAGES)
    cache_c_out = flat_c.at[dest_rows].set(new_c.reshape(REQUESTS * CHUNK_PAGES, PAGE_LEN, LATENT))
    cache_kr_out = flat_kr.at[dest_rows].set(new_kr.reshape(REQUESTS * CHUNK_PAGES, PAGE_LEN, ROPE_DIM))
    cache_c_out = cache_c_out.reshape(POOL_SIZE, CACHE_PAGES, PAGE_LEN, LATENT)
    cache_kr_out = cache_kr_out.reshape(POOL_SIZE, CACHE_PAGES, PAGE_LEN, ROPE_DIM)
    return hidden_out, cache_c_out, cache_kr_out
```

```python
import functools

import jax
import jax.numpy as jnp
from jax import lax
from jax.experimental import pallas as pl
from jax.experimental.pallas import tpu as pltpu
from jax.sharding import PartitionSpec as P

PAGE_LEN = 64
LATENT = 512
ROPE_DIM = 64
NOPE_DIM = 128
HEADS = 64
CHUNK = 64
D_MODEL = 7168
SLOTS = 4
NORM_EPS = 1e-6
ROPE_BASE = 10000.0
MESH = pl.DeviceIdType.MESH
VMEM_LIMIT = 62 * 1024 * 1024


def rope_tables(positions):
    half_dim = ROPE_DIM // 2
    inv_freq = ROPE_BASE ** (-jnp.arange(half_dim, dtype=jnp.float32) / half_dim)
    angles = positions.astype(jnp.float32)[..., None] * inv_freq
    return jnp.cos(angles), jnp.sin(angles)


def apply_rope(values, cos_tab, sin_tab):
    half_dim = ROPE_DIM // 2
    first = values[..., :half_dim]
    second = values[..., half_dim:]
    return jnp.concatenate([first * cos_tab - second * sin_tab, second * cos_tab + first * sin_tab], axis=-1)


def exchange_kernel(n, ids_ref, x_ref, cache_c, cache_kr, w_q, got_c, got_k, q_ref,
                    ids_in, ids_smem, cc, ck, kp, stage_c, stage_k, wbuf,
                    loc_sem, id_send, id_recv, c_send, c_recv, k_send, k_recv, w_sem, out_sem):
    me = lax.axis_index("pool")
    pages = kp.shape[0]
    blk = wbuf.shape[2]
    n_blk = w_q.shape[1] // blk

    load_c = pltpu.make_async_copy(cache_c.at[pl.ds(0, pages)], cc, loc_sem.at[0])
    load_k = pltpu.make_async_copy(cache_kr.at[pl.ds(0, pages)], ck, loc_sem.at[1])
    load_c.start()
    load_k.start()

    def peer_of(j):
        off = (j + 1) // 2
        sign = 1 - 2 * (j % 2)
        return (me + n // 2 + sign * off + n) % n

    barrier = pltpu.get_barrier_semaphore()

    @pl.loop(0, n - 1)
    def _(j):
        pl.semaphore_signal(barrier, inc=1, device_id=(peer_of(j),), device_id_type=MESH)

    def w_copy(i, slot):
        return pltpu.make_async_copy(w_q.at[:, pl.ds(pl.multiple_of(i * blk, blk), blk)], wbuf.at[slot], w_sem.at[slot])

    w_copy(0, 0).start()
    w_copy(1, 1).start()
    pl.semaphore_wait(barrier, n - 1)

    def id_copy(peer, src):
        return pltpu.make_async_remote_copy(src_ref=ids_ref.at[peer], dst_ref=ids_in.at[src], send_sem=id_send.at[peer],
                                            recv_sem=id_recv.at[src], device_id=(peer,), device_id_type=MESH)

    @pl.loop(0, n - 1)
    def _(j):
        id_copy(peer_of(j), me).start()

    own_ids = pltpu.make_async_copy(ids_ref.at[me], ids_in.at[me], loc_sem.at[2])
    own_ids.start()

    load_k.wait()

    @pl.loop(0, pages)
    def _(i):
        page = ck[i]
        kp[i] = jnp.concatenate([page[: PAGE_LEN // 2], page[PAGE_LEN // 2:]], axis=-1)

    load_c.wait()
    own_ids.wait()

    @pl.loop(0, n - 1)
    def _(j):
        id_copy(peer_of(j), peer_of(j)).wait_recv()

    to_smem = pltpu.make_async_copy(ids_in, ids_smem, loc_sem.at[3])
    to_smem.start()
    to_smem.wait()

    def c_copy(peer, src):
        return pltpu.make_async_remote_copy(src_ref=stage_c.at[peer], dst_ref=got_c.at[src], send_sem=c_send.at[peer],
                                            recv_sem=c_recv.at[src], device_id=(peer,), device_id_type=MESH)

    def k_copy(peer, src):
        return pltpu.make_async_remote_copy(src_ref=stage_k.at[peer], dst_ref=got_k.at[src], send_sem=k_send.at[peer],
                                            recv_sem=k_recv.at[src], device_id=(peer,), device_id_type=MESH)

    def fill(peer):
        for s in range(SLOTS):
            page = ids_smem[peer, 0, s]
            stage_c[peer, s] = cc[page]
            stage_k[peer, s] = kp[page]

    @pl.loop(0, n - 1)
    def _(j):
        peer = peer_of(j)
        fill(peer)
        c_copy(peer, me).start()
        k_copy(peer, me).start()

    fill(me)
    own_c = pltpu.make_async_copy(stage_c.at[me], got_c.at[me], out_sem.at[0])
    own_k = pltpu.make_async_copy(stage_k.at[me], got_k.at[me], out_sem.at[1])
    own_c.start()
    own_k.start()

    @pl.loop(0, n_blk // 2)
    def _(g):
        for slot in range(2):
            i = g * 2 + slot
            w_copy(i, slot).wait()
            part = jnp.dot(x_ref[...], wbuf[slot], preferred_element_type=jnp.float32)
            q_ref[:, pl.ds(pl.multiple_of(i * blk, blk), blk)] = part.astype(jnp.bfloat16)

            @pl.when(i + 2 < n_blk)
            def _():
                w_copy(i + 2, slot).start()

    own_c.wait()
    own_k.wait()

    @pl.loop(0, n - 1)
    def _(j):
        peer = peer_of(j)
        id_copy(peer, me).wait_send()
        c_copy(peer, peer).wait()
        k_copy(peer, peer).wait()


def exchange(n, ids, x, cache_c, cache_kr, w_q):
    pages = cache_c.shape[0] - 1
    blk = 256
    any_spec = pl.BlockSpec(memory_space=pl.ANY)
    vmem_spec = pl.BlockSpec(memory_space=pltpu.VMEM)
    return pl.pallas_call(
        functools.partial(exchange_kernel, n),
        name="exchange",
        out_shape=(
            jax.ShapeDtypeStruct((n, SLOTS, PAGE_LEN, LATENT), jnp.bfloat16),
            jax.ShapeDtypeStruct((n, SLOTS, PAGE_LEN // 2, 2 * ROPE_DIM), jnp.bfloat16),
            jax.ShapeDtypeStruct((CHUNK, w_q.shape[1]), jnp.bfloat16),
        ),
        in_specs=[vmem_spec, vmem_spec, any_spec, any_spec, any_spec],
        out_specs=(any_spec, any_spec, vmem_spec),
        scratch_shapes=[
            pltpu.VMEM((n, 1, 128), jnp.int32),
            pltpu.SMEM((n, 1, 128), jnp.int32),
            pltpu.VMEM((pages, PAGE_LEN, LATENT), jnp.bfloat16),
            pltpu.VMEM((pages, PAGE_LEN, ROPE_DIM), jnp.bfloat16),
            pltpu.VMEM((pages, PAGE_LEN // 2, 2 * ROPE_DIM), jnp.bfloat16),
            pltpu.VMEM((n, SLOTS, PAGE_LEN, LATENT), jnp.bfloat16),
            pltpu.VMEM((n, SLOTS, PAGE_LEN // 2, 2 * ROPE_DIM), jnp.bfloat16),
            pltpu.VMEM((2, D_MODEL, blk), jnp.bfloat16),
            pltpu.SemaphoreType.DMA((4,)),
            pltpu.SemaphoreType.DMA((n,)),
            pltpu.SemaphoreType.DMA((n,)),
            pltpu.SemaphoreType.DMA((n,)),
            pltpu.SemaphoreType.DMA((n,)),
            pltpu.SemaphoreType.DMA((n,)),
            pltpu.SemaphoreType.DMA((n,)),
            pltpu.SemaphoreType.DMA((2,)),
            pltpu.SemaphoreType.DMA((2,)),
        ],
        compiler_params=pltpu.CompilerParams(collective_id=0, has_side_effects=True, vmem_limit_bytes=VMEM_LIMIT),
    )(ids, x, cache_c, cache_kr, w_q)


def slot_positions(owners, pool_size, slot_count):
    dev_ids = jnp.arange(pool_size, dtype=jnp.int32)
    owner_hits = (owners[:, None] == dev_ids[None, :]).astype(jnp.int32)
    tri = (jnp.arange(owners.shape[0])[:, None] > jnp.arange(owners.shape[0])[None, :]).astype(jnp.float32)
    earlier = jnp.dot(tri, owner_hits.astype(jnp.float32)).astype(jnp.int32)
    slot_rank = jnp.sum(earlier * owner_hits, axis=1)
    return jnp.where(owners >= 0, owners * slot_count + slot_rank, pool_size * slot_count)


def attend_kernel(keys_tile, valid_ref, qc_ref, qk_ref, got_c, got_k, newc_ref, newk_ref, o_ref, m_ref, l_ref, acc_ref, cbuf, kbuf, sem):
    scale = (NOPE_DIM + ROPE_DIM) ** -0.5
    count = valid_ref[0]
    per = keys_tile // PAGE_LEN
    rows = qc_ref.shape[0]
    n_tiles = (count + per - 1) // per

    def copies(t, slot, s):
        page = valid_ref[1 + jnp.minimum(t * per + s, count - 1)]
        return (pltpu.make_async_copy(got_c.at[page], cbuf.at[slot, s], sem.at[slot, s, 0]),
                pltpu.make_async_copy(got_k.at[page], kbuf.at[slot, s], sem.at[slot, s, 1]))

    def start(t, slot):
        for s in range(per):
            for c in copies(t, slot, s):
                c.start()

    def scores(qc, qk, ck, kk):
        dims = (((1,), (1,)), ((), ()))
        s = lax.dot_general(qc, ck, dims, preferred_element_type=jnp.float32)
        return (s + lax.dot_general(qk, kk, dims, preferred_element_type=jnp.float32)) * scale

    @pl.when(n_tiles > 0)
    def _():
        start(0, 0)

    causal = (lax.broadcasted_iota(jnp.int32, (rows, CHUNK), 1) <= lax.broadcasted_iota(jnp.int32, (rows, CHUNK), 0) % CHUNK)
    s = scores(qc_ref[...], qk_ref[:, :ROPE_DIM], newc_ref[...], newk_ref[...])
    s = jnp.where(causal, s, -jnp.inf)
    m = jnp.max(s, axis=-1, keepdims=True)
    p = jnp.exp(s - m)
    m_ref[...] = jnp.broadcast_to(m, m_ref.shape)
    l_ref[...] = jnp.broadcast_to(jnp.sum(p, axis=-1, keepdims=True), l_ref.shape)
    acc_ref[...] = jnp.dot(p.astype(jnp.bfloat16), newc_ref[...], preferred_element_type=jnp.float32)

    low = lax.broadcasted_iota(jnp.int32, (PAGE_LEN // 2, 2 * ROPE_DIM), 1) < ROPE_DIM

    def body(t, _):
        slot = lax.rem(t, 2)

        @pl.when(t + 1 < n_tiles)
        def _():
            start(t + 1, 1 - slot)

        for s in range(per):
            for c in copies(t, slot, s):
                c.wait()
        ck = cbuf[slot].reshape(keys_tile, LATENT)
        parts = []
        for s in range(per):
            page = kbuf[slot, s]
            zero = jnp.zeros_like(page)
            parts += [jnp.where(low, page, zero), jnp.where(low, zero, page)]
        kk = jnp.concatenate(parts, axis=0)
        sc = scores(qc_ref[...], qk_ref[...], ck, kk)
        key_ids = t * keys_tile + lax.broadcasted_iota(jnp.int32, sc.shape, 1)
        sc = jnp.where(key_ids < count * PAGE_LEN, sc, -jnp.inf)
        m_old = m_ref[:, :1]
        m_new = jnp.maximum(m_old, jnp.max(sc, axis=-1, keepdims=True))
        alpha = jnp.exp(m_old - m_new)
        p = jnp.exp(sc - m_new)
        m_ref[...] = jnp.broadcast_to(m_new, m_ref.shape)
        l_ref[...] = l_ref[...] * alpha + jnp.sum(p, axis=-1, keepdims=True)
        acc_ref[...] = acc_ref[...] * alpha + jnp.dot(p.astype(jnp.bfloat16), ck, preferred_element_type=jnp.float32)
        return 0

    lax.fori_loop(0, n_tiles, body, 0)
    o_ref[...] = (acc_ref[...] / l_ref[:, :1]).astype(jnp.bfloat16)


def attend(valid, qc, qk, got_c, got_k, new_c, new_k):
    total = qc.shape[0]
    rows = 512
    keys_tile = 512
    per = keys_tile // PAGE_LEN
    any_spec = pl.BlockSpec(memory_space=pl.ANY)
    return pl.pallas_call(
        functools.partial(attend_kernel, keys_tile),
        name="attend",
        grid=(total // rows,),
        out_shape=jax.ShapeDtypeStruct((total, LATENT), jnp.bfloat16),
        in_specs=[
            pl.BlockSpec(memory_space=pltpu.SMEM),
            pl.BlockSpec((rows, LATENT), lambda i: (i, 0)),
            pl.BlockSpec((rows, 2 * ROPE_DIM), lambda i: (i, 0)),
            any_spec,
            any_spec,
            pl.BlockSpec((CHUNK, LATENT), lambda i: (0, 0)),
            pl.BlockSpec((CHUNK, ROPE_DIM), lambda i: (0, 0)),
        ],
        out_specs=pl.BlockSpec((rows, LATENT), lambda i: (i, 0)),
        scratch_shapes=[
            pltpu.VMEM((rows, 128), jnp.float32),
            pltpu.VMEM((rows, 128), jnp.float32),
            pltpu.VMEM((rows, LATENT), jnp.float32),
            pltpu.VMEM((2, per, PAGE_LEN, LATENT), jnp.bfloat16),
            pltpu.VMEM((2, per, PAGE_LEN // 2, 2 * ROPE_DIM), jnp.bfloat16),
            pltpu.SemaphoreType.DMA((2, per, 2)),
        ],
        compiler_params=pltpu.CompilerParams(dimension_semantics=("arbitrary",), vmem_limit_bytes=VMEM_LIMIT),
    )(valid, qc, qk, got_c, got_k, new_c, new_k)


def write_new_pages(n, new_c, new_k, write_owner, cache_c, cache_kr):
    rows = jnp.concatenate([new_c, new_k], axis=-1).reshape(n, CHUNK // n, LATENT + ROPE_DIM)
    mark = jnp.broadcast_to(write_owner, (n, 1))
    owners = lax.all_to_all(mark, "pool", 0, 0, tiled=True)[:, 0]
    parts = lax.all_to_all(rows, "pool", 0, 0, tiled=True)
    order = jnp.sum(jnp.where(owners[None, :] == jnp.arange(n)[:, None], jnp.arange(n)[None, :], 0), axis=1)
    page = lax.all_to_all(parts[order], "pool", 0, 0, tiled=True).reshape(CHUNK, LATENT + ROPE_DIM)
    out_c = lax.dynamic_update_slice(cache_c, page[None, None, :, :LATENT], (0, cache_c.shape[1] - 1, 0, 0))
    out_kr = lax.dynamic_update_slice(cache_kr, page[None, None, :, LATENT:], (0, cache_kr.shape[1] - 1, 0, 0))
    return out_c, out_kr


def solution(mesh):
    n = mesh.shape["pool"]

    def device_step(hidden, pre_len, pre_table, wr_table, cache_c, cache_kr, w_q, w_dkv, g_kv, w_uk, w_uv, w_o):
        x = hidden[0]
        owners = pre_table[0, :, 0]
        pos = slot_positions(owners, n, SLOTS)
        slot_ids = jnp.arange(n * SLOTS, dtype=jnp.int32)
        hit = pos[None, :] == slot_ids[:, None]
        asked = jnp.sum(jnp.where(hit, pre_table[0, :, 1][None, :], 0), axis=1)
        ids = jnp.pad(asked.reshape(n, 1, SLOTS), ((0, 0), (0, 0), (0, 128 - SLOTS)))
        got_c, got_k, q_all = exchange(n, ids, x, cache_c[0], cache_kr[0], w_q)
        got_c = got_c.reshape(n * SLOTS, PAGE_LEN, LATENT)
        got_k = got_k.reshape(n * SLOTS, PAGE_LEN // 2, 2 * ROPE_DIM)
        valid = jnp.concatenate([pre_len // PAGE_LEN, jnp.minimum(pos, n * SLOTS - 1)]).astype(jnp.int32)

        kv_lat = jnp.dot(x, w_dkv, preferred_element_type=jnp.float32)
        lat_part = kv_lat[:, :LATENT]
        inv_rms = lax.rsqrt(jnp.mean(lat_part * lat_part, axis=-1, keepdims=True) + NORM_EPS)
        c_new = (lat_part * inv_rms * g_kv.astype(jnp.float32)).astype(jnp.bfloat16)
        cos_tab, sin_tab = rope_tables(pre_len[0] + jnp.arange(CHUNK))
        kr_new = apply_rope(kv_lat[:, LATENT:], cos_tab, sin_tab).astype(jnp.bfloat16)
        out_c, out_kr = write_new_pages(n, c_new, kr_new, wr_table[0, 0, 0], cache_c, cache_kr)

        q_all = q_all.reshape(CHUNK, HEADS, NOPE_DIM + ROPE_DIM)
        q_rope = apply_rope(q_all[..., NOPE_DIM:].astype(jnp.float32), cos_tab[:, None, :], sin_tab[:, None, :]).astype(jnp.bfloat16)
        q_lat = jnp.einsum("chn,lhn->hcl", q_all[..., :NOPE_DIM], w_uk, preferred_element_type=jnp.float32).astype(jnp.bfloat16)
        q_rope = q_rope.transpose(1, 0, 2).reshape(HEADS * CHUNK, ROPE_DIM)
        q_dup = jnp.concatenate([q_rope, q_rope], axis=-1)
        o_lat = attend(valid, q_lat.reshape(HEADS * CHUNK, LATENT), q_dup, got_c, got_k, c_new, kr_new)
        o_lat = o_lat.reshape(HEADS, CHUNK, LATENT)
        o_heads = jnp.einsum("hcl,lhv->chv", o_lat, w_uv, preferred_element_type=jnp.float32).astype(jnp.bfloat16)
        attn_out = jnp.dot(o_heads.reshape(CHUNK, -1), w_o, preferred_element_type=jnp.float32)
        y = (x.astype(jnp.float32) + attn_out).astype(jnp.bfloat16)
        return y[None], out_c, out_kr

    row_spec = P("pool")
    rep_spec = P()
    return jax.shard_map(device_step, mesh=mesh, in_specs=(row_spec,) * 6 + (rep_spec,) * 6, out_specs=(row_spec,) * 3, check_vma=False)
```

```python
import functools

import jax
import jax.numpy as jnp
from jax import lax
from jax.experimental import pallas as pl
from jax.experimental.pallas import tpu as pltpu
from jax.sharding import PartitionSpec as P

PAGE_LEN = 64
LATENT = 512
ROPE_DIM = 64
NOPE_DIM = 128
VALUE_DIM = 128
HEADS = 64
CHUNK = 64
D_MODEL = 7168
SLOTS = 4
NORM_EPS = 1e-6
ROPE_BASE = 10000.0
MESH = pl.DeviceIdType.MESH
VMEM_LIMIT = 63 * 1024 * 1024
SCALE2 = (NOPE_DIM + ROPE_DIM) ** -0.5 * 1.4426950408889634
ROWS = HEADS * CHUNK
SUB = 256
SUBS = 4
W_BLK = 256
KV_ROWS = 896
H_BLK = 8
LAST_DIMS = (((1,), (1,)), ((), ()))
BF16 = jnp.bfloat16
F32 = jnp.float32


def xor(a, b, bits):
    out = 0
    for i in range(bits):
        w = 2 ** i
        out = out + w * (((a // w) % 2 + (b // w) % 2) % 2)
    return out


def step_code(k):
    return k // 2 + 16 * (k % 2)


def rope(values, cos2, sin2):
    half = ROPE_DIM // 2
    swapped = jnp.concatenate([values[:, half:], values[:, :half]], axis=-1)
    return values * cos2 + swapped * sin2


def layer_kernel(n, ids_ref, x_ref, bias_ref, rot_ref, gain_ref, cache_c, cache_kr, w_q, w_dkv, w_uk, w_uv,
                 o_lat, wuv_out, page_c_out, page_k_out,
                 ids_in, ids_smem, cc, ck, kp, stage_c, stage_k, land_c, land_k, wbuf, q_all, qc, qk, m_ref, l_ref, acc,
                 hbuf, h32, hout, kvbuf, new_c, new_k, kk, part_out, part_mid, part_fwd, part_in, c32,
                 loc_sem, id_send, id_recv, c_send, c_recv, k_send, k_recv, p_send, p_recv, f_send, f_recv, w_sem, h_sem, ho_sem, kv_sem, out_sem):
    me = lax.axis_index("pool")
    bits = n.bit_length() - 1
    pages = kp.shape[0]
    n_blk = w_q.shape[1] // W_BLK
    n_kv = D_MODEL // KV_ROWS
    n_h = HEADS // H_BLK

    load_c = pltpu.make_async_copy(cache_c.at[pl.ds(0, pages)], cc, loc_sem.at[0])
    load_k = pltpu.make_async_copy(cache_kr.at[pl.ds(0, pages)], ck, loc_sem.at[1])
    load_k.start()
    load_c.start()

    def peer_of(k):
        return xor(me, step_code(k), bits)

    barrier = pltpu.get_barrier_semaphore()

    @pl.loop(1, n)
    def _(k):
        pl.semaphore_signal(barrier, inc=1, device_id=(peer_of(k),), device_id_type=MESH)

    def kv_copy(i, slot):
        return pltpu.make_async_copy(w_dkv.at[pl.ds(pl.multiple_of(i * KV_ROWS, KV_ROWS), KV_ROWS)], kvbuf.at[slot], kv_sem.at[slot])

    def w_copy(i, slot):
        return pltpu.make_async_copy(w_q.at[:, pl.ds(pl.multiple_of(i * W_BLK, W_BLK), W_BLK)], wbuf.at[slot], w_sem.at[slot])

    kv_copy(0, 0).start()
    kv_copy(1, 1).start()
    pl.semaphore_wait(barrier, n - 1)

    def id_copy(k):
        peer = peer_of(k)
        return pltpu.make_async_remote_copy(src_ref=ids_ref.at[peer], dst_ref=ids_in.at[k], send_sem=id_send.at[k],
                                            recv_sem=id_recv.at[k], device_id=(peer,), device_id_type=MESH)

    @pl.loop(1, n)
    def _(k):
        id_copy(k).start()

    own_ids = pltpu.make_async_copy(ids_ref.at[me], ids_in.at[0], loc_sem.at[2])
    own_ids.start()
    load_k.wait()

    @pl.loop(0, pages)
    def _(i):
        page = ck[i]
        kp[i] = jnp.concatenate([page[: PAGE_LEN // 2], page[PAGE_LEN // 2:]], axis=-1)

    load_c.wait()
    own_ids.wait()

    @pl.loop(1, n)
    def _(k):
        id_copy(k).wait_recv()

    to_smem = pltpu.make_async_copy(ids_in, ids_smem, loc_sem.at[3])
    to_smem.start()
    to_smem.wait()

    def c_copy(k):
        return pltpu.make_async_remote_copy(src_ref=stage_c.at[k], dst_ref=land_c.at[k], send_sem=c_send.at[k],
                                            recv_sem=c_recv.at[k], device_id=(peer_of(k),), device_id_type=MESH)

    def k_copy(k):
        return pltpu.make_async_remote_copy(src_ref=stage_k.at[k], dst_ref=land_k.at[k], send_sem=k_send.at[k],
                                            recv_sem=k_recv.at[k], device_id=(peer_of(k),), device_id_type=MESH)

    def send_pages(k):
        for s in range(SLOTS):
            page = ids_smem[k, 0, s]
            stage_c[k, s] = cc[page]
            stage_k[k, s] = kp[page]
        c_copy(k).start()
        k_copy(k).start()

    @pl.loop(1, n // 2)
    def _(k):
        send_pages(k)

    w_copy(0, 0).start()
    w_copy(1, 1).start()

    kv = jnp.zeros((CHUNK, LATENT + ROPE_DIM), F32)
    for i in range(n_kv):
        kv_copy(i, i % 2).wait()
        kv = kv + jnp.dot(x_ref[:, i * KV_ROWS:(i + 1) * KV_ROWS], kvbuf[i % 2], preferred_element_type=F32)
        if i + 2 < n_kv:
            kv_copy(i + 2, i % 2).start()
    lat = kv[:, :LATENT]
    inv_rms = lax.rsqrt(jnp.mean(lat * lat, axis=-1, keepdims=True) + NORM_EPS)
    c_new = (lat * inv_rms * gain_ref[...]).astype(BF16)
    cos2 = rot_ref[0]
    sin2 = rot_ref[1]
    kr_new = rope(kv[:, LATENT:], cos2, sin2).astype(BF16)
    new_c[...] = c_new
    new_k[...] = kr_new

    for g in range(LATENT // 128):
        c32[:, g, :] = c_new[:, g * 128:(g + 1) * 128].astype(F32)
    c32[:, 4, :] = jnp.concatenate([kr_new, kr_new], axis=-1).astype(F32)
    low = lax.broadcasted_iota(jnp.int32, (1, 128), 1) < ROPE_DIM
    for i in range(n):
        a = c32[2 * i]
        b = c32[2 * i + 1]
        last = jnp.where(low, a[4:5], b[4:5])
        part_out[i] = jnp.concatenate([a[:4], b[:4], jnp.broadcast_to(last, (8, 128))], axis=0).astype(BF16)

    def p_copy(k):
        peer = peer_of(k)
        return pltpu.make_async_remote_copy(src_ref=part_out.at[peer], dst_ref=part_mid.at[k], send_sem=p_send.at[k],
                                            recv_sem=p_recv.at[k], device_id=(peer,), device_id_type=MESH)

    def f_copy(k):
        peer = peer_of(k)
        return pltpu.make_async_remote_copy(src_ref=part_fwd.at[k], dst_ref=part_in.at[me], send_sem=f_send.at[k],
                                            recv_sem=f_recv.at[k], device_id=(peer,), device_id_type=MESH)

    def f_arrival(k):
        peer = peer_of(k)
        return pltpu.make_async_remote_copy(src_ref=part_fwd.at[k], dst_ref=part_in.at[peer], send_sem=f_send.at[k],
                                            recv_sem=f_recv.at[k], device_id=(peer,), device_id_type=MESH)

    @pl.loop(1, n)
    def _(k):
        p_copy(k).start()

    part_mid[0] = part_out[me]

    @pl.loop(n // 2, n)
    def _(k):
        send_pages(k)

    for s in range(SLOTS):
        page = ids_smem[0, 0, s]
        land_c[0, s] = cc[page]
        land_k[0, s] = kp[page]

    @pl.loop(0, n_blk // 2)
    def _(g):
        for slot in range(2):
            i = g * 2 + slot
            w_copy(i, slot).wait()
            part = jnp.dot(x_ref[...], wbuf[slot], preferred_element_type=F32)
            q_all[:, pl.ds(pl.multiple_of(i * W_BLK, W_BLK), W_BLK)] = part.astype(BF16)

            @pl.when(i + 2 < n_blk)
            def _():
                w_copy(i + 2, slot).start()

    def h_copy(src, i, slot):
        return pltpu.make_async_copy(src.at[:, pl.ds(pl.multiple_of(i * H_BLK, H_BLK), H_BLK)], hbuf.at[slot], h_sem.at[slot])

    h_copy(w_uk, 0, 0).start()

    @pl.loop(0, n_h)
    def _(i):
        slot = i % 2
        h_copy(w_uk, i, slot).wait()

        @pl.when(i + 1 < n_h)
        def _():
            h_copy(w_uk, i + 1, 1 - slot).start()

        h32[...] = hbuf[slot].astype(F32)
        for pair in range(H_BLK // 2):
            q2 = q_all[:, pl.ds(pl.multiple_of((i * (H_BLK // 2) + pair) * 384, 128), 384)]
            q32 = q2.astype(F32)
            for odd in range(2):
                j = pair * 2 + odd
                base = odd * (NOPE_DIM + ROPE_DIM)
                wk = h32[:, j, :].astype(BF16)
                u = lax.dot_general(q2[:, base:base + NOPE_DIM], wk, LAST_DIMS, preferred_element_type=F32)
                qr = rope(q32[:, base + NOPE_DIM:base + NOPE_DIM + ROPE_DIM], cos2, sin2).astype(BF16)
                at = pl.ds(pl.multiple_of((i * H_BLK + j) * CHUNK, CHUNK), CHUNK)
                qc[at, :] = u.astype(BF16)
                qk[at, :] = jnp.concatenate([qr, qr], axis=-1)

    def ho_copy(i):
        return pltpu.make_async_copy(hout, wuv_out.at[pl.ds(pl.multiple_of(i * H_BLK, H_BLK), H_BLK)], ho_sem.at[0])

    h_copy(w_uv, 0, 0).start()

    @pl.loop(0, n_h)
    def _(i):
        slot = i % 2
        h_copy(w_uv, i, slot).wait()

        @pl.when(i + 1 < n_h)
        def _():
            h_copy(w_uv, i + 1, 1 - slot).start()

        h32[...] = hbuf[slot].astype(F32)

        @pl.when(i > 0)
        def _():
            ho_copy(i - 1).wait()

        for j in range(H_BLK):
            hout[j] = h32[:, j, :].astype(BF16)
        ho_copy(i).start()

    def tile(at, s, keys):
        m_old = m_ref[at, :]
        m_new = jnp.maximum(m_old, jnp.max(s, axis=-1, keepdims=True))
        alpha = jnp.exp2(m_old - m_new)
        groups = s.shape[1] // 128
        parts = [jnp.exp2(s[:, g * 128:(g + 1) * 128] - m_new) for g in range(groups)]
        total = parts[0]
        for p in parts[1:]:
            total = total + p
        m_ref[at, :] = m_new
        l_ref[at, :] = l_ref[at, :] * alpha + total
        p = jnp.concatenate([p.astype(BF16) for p in parts], axis=-1)
        pv = jnp.dot(p, keys, preferred_element_type=F32)
        for g in range(LATENT // 128):
            lanes = slice(g * 128, (g + 1) * 128)
            acc[at, lanes] = acc[at, lanes] * alpha + pv[:, lanes]

    first_lanes = lax.broadcasted_iota(jnp.int32, (CHUNK, 2 * ROPE_DIM), 1) < ROPE_DIM

    @pl.loop(0, ROWS // SUB)
    def _(i):
        at = pl.ds(pl.multiple_of(i * SUB, SUB), SUB)
        causal = (lax.broadcasted_iota(jnp.int32, (SUB, CHUNK), 1) <= lax.broadcasted_iota(jnp.int32, (SUB, CHUNK), 0) % CHUNK)
        k64 = jnp.concatenate([new_k[...], jnp.zeros((CHUNK, ROPE_DIM), BF16)], axis=-1)
        s = lax.dot_general(qc[at, :], new_c[...], LAST_DIMS, preferred_element_type=F32)
        s = s + lax.dot_general(qk[at, :], k64, LAST_DIMS, preferred_element_type=F32)
        s = jnp.where(causal, s * SCALE2, -jnp.inf)
        m = jnp.max(s, axis=-1, keepdims=True)
        p = jnp.exp2(s - m)
        m_ref[at, :] = jnp.broadcast_to(m, (SUB, 128))
        l_ref[at, :] = jnp.concatenate([p, jnp.zeros((SUB, 128 - CHUNK), F32)], axis=-1)
        acc[at, :] = jnp.dot(p.astype(BF16), new_c[...], preferred_element_type=F32)

    half_low = lax.broadcasted_iota(jnp.int32, (PAGE_LEN // 2, 2 * ROPE_DIM), 1) < ROPE_DIM

    @pl.loop(0, n // 2)
    def _(t):
        @pl.when(t > 0)
        def _():
            c_copy(2 * t).wait_recv()
            k_copy(2 * t).wait_recv()

        c_copy(2 * t + 1).wait_recv()
        k_copy(2 * t + 1).wait_recv()

        for d in range(2):
            for s in range(SLOTS):
                page = land_k[2 * t + d, s]
                zero = jnp.zeros_like(page)
                base = (d * SLOTS + s) * PAGE_LEN
                kk[base:base + PAGE_LEN // 2, :] = jnp.where(half_low, page, zero)
                kk[base + PAGE_LEN // 2:base + PAGE_LEN, :] = jnp.where(half_low, zero, page)

        @pl.loop(0, ROWS // (SUB * SUBS))
        def _(i):
            keys = land_c[pl.ds(2 * t, 2)].reshape(2 * SLOTS * PAGE_LEN, LATENT)
            bias = bias_ref[t]
            ats = [pl.ds(pl.multiple_of((i * SUBS + u) * SUB, SUB), SUB) for u in range(SUBS)]
            raw = []
            for at in ats:
                s = lax.dot_general(qc[at, :], keys, LAST_DIMS, preferred_element_type=F32)
                raw.append(s + lax.dot_general(qk[at, :], kk[...], LAST_DIMS, preferred_element_type=F32))
            for at, s in zip(ats, raw):
                tile(at, s * SCALE2 + bias, keys)

        @pl.when(t == n // 2 - 6)
        def _():
            @pl.loop(1, n)
            def _(k):
                p_copy(k).wait_recv()

            @pl.loop(0, n)
            def _(k):
                owner = peer_of(k)
                source = jnp.int32(0)
                for j in range(n):
                    source = jnp.where(ids_smem[j, 0, SLOTS] == owner, j, source)
                part_fwd[k] = part_mid[source]

            @pl.loop(1, n)
            def _(k):
                f_copy(k).start()

            part_in[me] = part_fwd[0]

    @pl.loop(0, ROWS // SUB)
    def _(i):
        at = pl.ds(pl.multiple_of(i * SUB, SUB), SUB)
        total = jnp.sum(l_ref[at, :], axis=-1, keepdims=True)
        qc[at, :] = (acc[at, :] / total).astype(BF16)

    out = pltpu.make_async_copy(qc, o_lat, out_sem.at[0])
    out.start()

    @pl.loop(1, n)
    def _(k):
        f_arrival(k).wait_recv()

    for i in range(n):
        part = part_in[i].astype(F32)
        c32[2 * i, 0:4] = part[0:4]
        c32[2 * i + 1, 0:4] = part[4:8]
        c32[2 * i, 4:5] = part[8:9]
        c32[2 * i + 1, 4:5] = jnp.concatenate([part[8:9, ROPE_DIM:], part[8:9, :ROPE_DIM]], axis=-1)
    for g in range(LATENT // 128):
        new_c[:, g * 128:(g + 1) * 128] = c32[:, g, :].astype(BF16)
    new_k[...] = c32[:, 4, :][:, :ROPE_DIM].astype(BF16)
    out_pc = pltpu.make_async_copy(new_c, page_c_out, out_sem.at[1])
    out_pk = pltpu.make_async_copy(new_k, page_k_out, out_sem.at[2])
    out_pc.start()
    out_pk.start()

    @pl.loop(1, n)
    def _(k):
        id_copy(k).wait_send()
        c_copy(k).wait_send()
        k_copy(k).wait_send()
        p_copy(k).wait_send()
        f_copy(k).wait_send()

    ho_copy(n_h - 1).wait()
    out.wait()
    out_pc.wait()
    out_pk.wait()


def layer(n, ids, x, bias, rot, gain, cache_c, cache_kr, w_q, w_dkv, w_uk, w_uv):
    pages = cache_c.shape[0] - 1
    any_spec = pl.BlockSpec(memory_space=pl.ANY)
    vmem = pl.BlockSpec(memory_space=pltpu.VMEM)
    dma = pltpu.SemaphoreType.DMA
    return pl.pallas_call(
        functools.partial(layer_kernel, n),
        name="layer",
        out_shape=(
            jax.ShapeDtypeStruct((ROWS, LATENT), BF16),
            jax.ShapeDtypeStruct((HEADS, LATENT, VALUE_DIM), BF16),
            jax.ShapeDtypeStruct((CHUNK, LATENT), BF16),
            jax.ShapeDtypeStruct((CHUNK, ROPE_DIM), BF16),
        ),
        in_specs=[vmem] * 5 + [any_spec] * 6,
        out_specs=(any_spec,) * 4,
        scratch_shapes=[
            pltpu.VMEM((n, 1, 128), jnp.int32),
            pltpu.SMEM((n, 1, 128), jnp.int32),
            pltpu.VMEM((pages, PAGE_LEN, LATENT), BF16),
            pltpu.VMEM((pages, PAGE_LEN, ROPE_DIM), BF16),
            pltpu.VMEM((pages, PAGE_LEN // 2, 2 * ROPE_DIM), BF16),
            pltpu.VMEM((n, SLOTS, PAGE_LEN, LATENT), BF16),
            pltpu.VMEM((n, SLOTS, PAGE_LEN // 2, 2 * ROPE_DIM), BF16),
            pltpu.VMEM((n, SLOTS, PAGE_LEN, LATENT), BF16),
            pltpu.VMEM((n, SLOTS, PAGE_LEN // 2, 2 * ROPE_DIM), BF16),
            pltpu.VMEM((2, D_MODEL, W_BLK), BF16),
            pltpu.VMEM((CHUNK, HEADS * (NOPE_DIM + ROPE_DIM)), BF16),
            pltpu.VMEM((ROWS, LATENT), BF16),
            pltpu.VMEM((ROWS, 2 * ROPE_DIM), BF16),
            pltpu.VMEM((ROWS, 128), F32),
            pltpu.VMEM((ROWS, 128), F32),
            pltpu.VMEM((ROWS, LATENT), F32),
            pltpu.VMEM((2, LATENT, H_BLK, NOPE_DIM), BF16),
            pltpu.VMEM((LATENT, H_BLK, NOPE_DIM), F32),
            pltpu.VMEM((H_BLK, LATENT, VALUE_DIM), BF16),
            pltpu.VMEM((2, KV_ROWS, LATENT + ROPE_DIM), BF16),
            pltpu.VMEM((CHUNK, LATENT), BF16),
            pltpu.VMEM((CHUNK, ROPE_DIM), BF16),
            pltpu.VMEM((2 * SLOTS * PAGE_LEN, 2 * ROPE_DIM), BF16),
            pltpu.VMEM((n, 16, 128), BF16),
            pltpu.VMEM((n, 16, 128), BF16),
            pltpu.VMEM((n, 16, 128), BF16),
            pltpu.VMEM((n, 16, 128), BF16),
            pltpu.VMEM((CHUNK, 8, 128), F32),
            dma((4,)),
        ] + [dma((n,))] * 10 + [dma((2,)), dma((2,)), dma((1,)), dma((2,)), dma((3,))],
        compiler_params=pltpu.CompilerParams(collective_id=0, has_side_effects=True, vmem_limit_bytes=VMEM_LIMIT),
    )(ids, x, bias, rot, gain, cache_c, cache_kr, w_q, w_dkv, w_uk, w_uv)


O_BLK = 256
O_BUFS = 6


def finish_kernel(x_ref, o_lat, wuv, w_o, cache_c, cache_kr, page_c, page_k, y_ref, out_c, out_kr,
                  lat, wv, heads, wbuf, cbuf, kbuf, lat_sem, wv_sem, w_sem, in_sem, out_sem):
    n_blk = w_o.shape[1] // O_BLK
    n_h = HEADS // H_BLK
    pages = cache_c.shape[0] - 1

    def lat_copy(i):
        at = pl.ds(pl.multiple_of(i * H_BLK * CHUNK, 8), H_BLK * CHUNK)
        return pltpu.make_async_copy(o_lat.at[at], lat.at[at], lat_sem.at[i])

    def wv_copy(i):
        at = pl.ds(pl.multiple_of(i * H_BLK, H_BLK), H_BLK)
        return pltpu.make_async_copy(wuv.at[at], wv.at[at], wv_sem.at[i])

    def w_copy(i, slot):
        return pltpu.make_async_copy(w_o.at[:, pl.ds(pl.multiple_of(i * O_BLK, O_BLK), O_BLK)], wbuf.at[slot], w_sem.at[slot])

    for i in range(n_h):
        lat_copy(i).start()
        wv_copy(i).start()
    ins = [pltpu.make_async_copy(cache_c.at[pl.ds(0, pages)], cbuf.at[pl.ds(0, pages)], in_sem.at[0]),
           pltpu.make_async_copy(cache_kr.at[pl.ds(0, pages)], kbuf.at[pl.ds(0, pages)], in_sem.at[1]),
           pltpu.make_async_copy(page_c, cbuf.at[pages], in_sem.at[2]),
           pltpu.make_async_copy(page_k, kbuf.at[pages], in_sem.at[3])]
    for i in range(O_BUFS):
        w_copy(i, i).start()
    for c in ins:
        c.start()

    @pl.loop(0, n_h)
    def _(i):
        lat_copy(i).wait()
        wv_copy(i).wait()
        for j in range(H_BLK):
            h = i * H_BLK + j
            o = jnp.dot(lat[pl.ds(pl.multiple_of(h * CHUNK, CHUNK), CHUNK), :], wv[h], preferred_element_type=F32)
            heads[:, pl.ds(pl.multiple_of(h * VALUE_DIM, VALUE_DIM), VALUE_DIM)] = o.astype(BF16)

    for c in ins:
        c.wait()
    outs = [pltpu.make_async_copy(cbuf, out_c, out_sem.at[0]), pltpu.make_async_copy(kbuf, out_kr, out_sem.at[1])]
    for c in outs:
        c.start()

    @pl.loop(0, n_blk)
    def _(i):
        slot = lax.rem(i, O_BUFS)
        w_copy(i, slot).wait()
        at = pl.ds(pl.multiple_of(i * O_BLK, O_BLK), O_BLK)
        part = jnp.dot(heads[...], wbuf[slot], preferred_element_type=F32)
        y_ref[:, at] = (x_ref[:, at].astype(F32) + part).astype(BF16)

        @pl.when(i + O_BUFS < n_blk)
        def _():
            w_copy(i + O_BUFS, slot).start()

    for c in outs:
        c.wait()


def finish(x, o_lat, wuv, w_o, cache_c, cache_kr, page_c, page_k):
    any_spec = pl.BlockSpec(memory_space=pl.ANY)
    vmem = pl.BlockSpec(memory_space=pltpu.VMEM)
    dma = pltpu.SemaphoreType.DMA
    n_h = HEADS // H_BLK
    return pl.pallas_call(
        finish_kernel,
        name="finish",
        out_shape=(
            jax.ShapeDtypeStruct(x.shape, BF16),
            jax.ShapeDtypeStruct(cache_c.shape, BF16),
            jax.ShapeDtypeStruct(cache_kr.shape, BF16),
        ),
        in_specs=[vmem] + [any_spec] * 7,
        out_specs=(vmem, any_spec, any_spec),
        scratch_shapes=[
            pltpu.VMEM(o_lat.shape, BF16),
            pltpu.VMEM(wuv.shape, BF16),
            pltpu.VMEM((CHUNK, HEADS * VALUE_DIM), BF16),
            pltpu.VMEM((O_BUFS, HEADS * VALUE_DIM, O_BLK), BF16),
            pltpu.VMEM(cache_c.shape, BF16),
            pltpu.VMEM(cache_kr.shape, BF16),
            dma((n_h,)),
            dma((n_h,)),
            dma((O_BUFS,)),
            dma((4,)),
            dma((2,)),
        ],
        compiler_params=pltpu.CompilerParams(vmem_limit_bytes=VMEM_LIMIT),
    )(x, o_lat, wuv, w_o, cache_c, cache_kr, page_c, page_k)


def solution(mesh):
    n = mesh.shape["pool"]

    def device_step(hidden, pre_len, pre_table, wr_table, cache_c, cache_kr, w_q, w_dkv, g_kv, w_uk, w_uv, w_o):
        x = hidden[0]
        me = lax.axis_index("pool")
        owners = pre_table[0, :, 0]
        table_pages = owners.shape[0]
        earlier = jnp.arange(table_pages)[:, None] > jnp.arange(table_pages)[None, :]
        rank = jnp.sum(jnp.where(earlier & (owners[:, None] == owners[None, :]), 1, 0), axis=1)
        pos = jnp.where(owners >= 0, owners * SLOTS + rank, -1)
        lanes = jnp.arange(128, dtype=jnp.int32)
        slot_of = jnp.where(lanes < SLOTS, jnp.arange(n, dtype=jnp.int32)[:, None] * SLOTS + lanes, -2)
        asked = jnp.sum(jnp.where(pos[None, None, :] == slot_of[:, :, None], pre_table[0, :, 1], 0), axis=2)
        ids = jnp.where(lanes == SLOTS, wr_table[0, 0, 0], asked)[:, None, :].astype(jnp.int32)
        keys = jnp.arange(2 * SLOTS * PAGE_LEN, dtype=jnp.int32)
        owner_of = jnp.bitwise_xor(me, jnp.arange(n // 2, dtype=jnp.int32)[:, None] + 16 * (keys // (SLOTS * PAGE_LEN)))
        counts = jnp.sum(jnp.where(owner_of[:, :: SLOTS * PAGE_LEN, None] == owners, 1, 0), axis=2)
        counts = jnp.repeat(counts, SLOTS * PAGE_LEN, axis=1)
        bias = jnp.where((keys // PAGE_LEN) % SLOTS < counts, 0.0, -jnp.inf).astype(F32)[:, None, :]
        cos_tab, sin_tab = rope_tables(pre_len[0] + jnp.arange(CHUNK))
        rot = jnp.stack([jnp.concatenate([cos_tab, cos_tab], -1), jnp.concatenate([-sin_tab, sin_tab], -1)])
        o_lat, wuv, page_c, page_k = layer(n, ids, x, bias, rot, g_kv.astype(F32)[None], cache_c[0], cache_kr[0], w_q, w_dkv, w_uk, w_uv)
        y, out_c, out_kr = finish(x, o_lat, wuv, w_o, cache_c[0], cache_kr[0], page_c, page_k)
        return y[None], out_c[None], out_kr[None]

    row_spec = P("pool")
    rep_spec = P()
    return jax.shard_map(device_step, mesh=mesh, in_specs=(row_spec,) * 6 + (rep_spec,) * 6, out_specs=(row_spec,) * 3, check_vma=False)


def rope_tables(positions):
    half_dim = ROPE_DIM // 2
    inv_freq = ROPE_BASE ** (-jnp.arange(half_dim, dtype=F32) / half_dim)
    angles = positions.astype(F32)[..., None] * inv_freq
    return jnp.cos(angles), jnp.sin(angles)
```

```python
import functools

import jax
import jax.numpy as jnp
from jax import lax
from jax.experimental import pallas as pl
from jax.experimental.pallas import tpu as pltpu
from jax.sharding import PartitionSpec as P

PAGE_LEN = 64
LATENT = 512
ROPE_DIM = 64
NOPE_DIM = 128
VALUE_DIM = 128
HEADS = 64
CHUNK = 64
D_MODEL = 7168
SLOTS = 4
NORM_EPS = 1e-6
ROPE_BASE = 10000.0
MESH = pl.DeviceIdType.MESH
VMEM_LIMIT = 63 * 1024 * 1024
SCALE2 = (NOPE_DIM + ROPE_DIM) ** -0.5 * 1.4426950408889634
ROWS = HEADS * CHUNK
SUB = 256
SUBS = 4
W_BLK = 512
W_ROWS = 1792
W_BUFS = 4
KV_ROWS = 896
H_BLK = 8
LAST_DIMS = (((1,), (1,)), ((), ()))
BF16 = jnp.bfloat16
F32 = jnp.float32


def step_code(k):
    return lax.div(k, 2) + 16 * lax.rem(k, 2)


def flip_weights(me, bits):
    return [2 ** i - 2 ** (i + 1) * lax.rem(lax.div(me, 2 ** i), 2) for i in range(bits)]


def flipped(me, flips, code):
    out = me
    for i, f in enumerate(flips):
        out = out + f * lax.rem(lax.div(code, 2 ** i), 2)
    return out


def rope(values, cos2, sin2):
    half = ROPE_DIM // 2
    swapped = jnp.concatenate([values[:, half:], values[:, :half]], axis=-1)
    return values * cos2 + swapped * sin2


def layer_kernel(n, ids_ref, x_ref, bias_ref, rot_ref, gain_ref, cache_c, cache_kr, w_q, w_dkv, w_uk, w_uv,
                 o_lat, wuv_out, page_c_out, page_k_out,
                 ids_in, ids_smem, cc, ck, kp, stage_c, stage_k, land_c, land_k, wbuf, q_all, qc, qk, m_ref, l_ref, acc,
                 hbuf, h32, hout, kvbuf, new_c, new_k, kk, part_out, part_mid, part_fwd, part_in, c32,
                 loc_sem, id_send, id_recv, c_send, c_recv, k_send, k_recv, p_send, p_recv, f_send, f_recv, w_sem, h_sem, ho_sem, kv_sem, out_sem):
    me = lax.axis_index("pool")
    bits = n.bit_length() - 1
    pages = kp.shape[0]
    n_blk = w_q.shape[1] // W_BLK
    n_kv = D_MODEL // KV_ROWS
    n_h = HEADS // H_BLK

    load_c = pltpu.make_async_copy(cache_c.at[pl.ds(0, pages)], cc, loc_sem.at[0])
    load_k = pltpu.make_async_copy(cache_kr.at[pl.ds(0, pages)], ck, loc_sem.at[1])
    load_k.start()
    load_c.start()

    flips = flip_weights(me, bits)
    any_peer = lax.rem(me + 1, n)

    def peer_of(k):
        return flipped(me, flips, step_code(k))

    barrier = pltpu.get_barrier_semaphore()

    @pl.loop(1, n)
    def _(k):
        pl.semaphore_signal(barrier, inc=1, device_id=(peer_of(k),), device_id_type=MESH)

    def kv_copy(i, slot):
        return pltpu.make_async_copy(w_dkv.at[:, pl.ds(i * KV_ROWS, KV_ROWS)], kvbuf.at[slot], kv_sem.at[slot])

    n_row = D_MODEL // W_ROWS

    def w_copy(col, r):
        rows = pl.ds(r * W_ROWS, W_ROWS)
        return pltpu.make_async_copy(w_q.at[rows, pl.ds(pl.multiple_of(col * W_BLK, W_BLK), W_BLK)], wbuf.at[r], w_sem.at[r])

    kv_copy(0, 0).start()
    kv_copy(1, 1).start()
    pl.semaphore_wait(barrier, n - 1)

    def id_copy(k, peer):
        return pltpu.make_async_remote_copy(src_ref=ids_ref.at[peer], dst_ref=ids_in.at[k], send_sem=id_send.at[k],
                                            recv_sem=id_recv.at[k], device_id=(peer,), device_id_type=MESH)

    @pl.loop(1, n)
    def _(k):
        id_copy(k, peer_of(k)).start()

    own_ids = pltpu.make_async_copy(ids_ref.at[me], ids_in.at[0], loc_sem.at[2])
    own_ids.start()
    load_k.wait()

    @pl.loop(0, pages)
    def _(i):
        page = ck[i]
        kp[i] = jnp.concatenate([page[: PAGE_LEN // 2], page[PAGE_LEN // 2:]], axis=-1)

    load_c.wait()
    own_ids.wait()

    @pl.loop(1, n)
    def _(k):
        id_copy(k, any_peer).wait_recv()

    to_smem = pltpu.make_async_copy(ids_in, ids_smem, loc_sem.at[3])
    to_smem.start()
    to_smem.wait()

    def c_copy(k, peer):
        return pltpu.make_async_remote_copy(src_ref=stage_c.at[k], dst_ref=land_c.at[k], send_sem=c_send.at[k],
                                            recv_sem=c_recv.at[k], device_id=(peer,), device_id_type=MESH)

    def k_copy(k, peer):
        return pltpu.make_async_remote_copy(src_ref=stage_k.at[k], dst_ref=land_k.at[k], send_sem=k_send.at[k],
                                            recv_sem=k_recv.at[k], device_id=(peer,), device_id_type=MESH)

    def send_pages(k):
        peer = peer_of(k)
        for s in range(SLOTS):
            page = ids_smem[k, 0, s]
            stage_c[k, s] = cc[page]
            stage_k[k, s] = kp[page]
        c_copy(k, peer).start()
        k_copy(k, peer).start()

    @pl.loop(1, n // 2)
    def _(k):
        send_pages(k)

    for r in range(n_row):
        w_copy(0, r).start()

    kv = jnp.zeros((CHUNK, LATENT + ROPE_DIM), F32)
    for i in range(n_kv):
        kv_copy(i, i % 2).wait()
        kv = kv + lax.dot_general(x_ref[:, i * KV_ROWS:(i + 1) * KV_ROWS], kvbuf[i % 2], LAST_DIMS, preferred_element_type=F32)
        if i + 2 < n_kv:
            kv_copy(i + 2, i % 2).start()
    lat = kv[:, :LATENT]
    inv_rms = lax.rsqrt(jnp.mean(lat * lat, axis=-1, keepdims=True) + NORM_EPS)
    c_new = (lat * inv_rms * gain_ref[...]).astype(BF16)
    cos2 = rot_ref[0]
    sin2 = rot_ref[1]
    kr_new = rope(kv[:, LATENT:], cos2, sin2).astype(BF16)
    new_c[...] = c_new
    new_k[...] = kr_new

    for g in range(LATENT // 128):
        c32[:, g, :] = c_new[:, g * 128:(g + 1) * 128].astype(F32)
    c32[:, 4, :] = jnp.concatenate([kr_new, kr_new], axis=-1).astype(F32)
    low = lax.broadcasted_iota(jnp.int32, (1, 128), 1) < ROPE_DIM
    for i in range(n):
        a = c32[2 * i]
        b = c32[2 * i + 1]
        last = jnp.where(low, a[4:5], b[4:5])
        part_out[i] = jnp.concatenate([a[:4], b[:4], jnp.broadcast_to(last, (8, 128))], axis=0).astype(BF16)

    def p_copy(k, peer):
        return pltpu.make_async_remote_copy(src_ref=part_out.at[peer], dst_ref=part_mid.at[k], send_sem=p_send.at[k],
                                            recv_sem=p_recv.at[k], device_id=(peer,), device_id_type=MESH)

    def f_copy(k, peer):
        return pltpu.make_async_remote_copy(src_ref=part_fwd.at[k], dst_ref=part_in.at[me], send_sem=f_send.at[k],
                                            recv_sem=f_recv.at[k], device_id=(peer,), device_id_type=MESH)

    @pl.loop(1, n)
    def _(k):
        p_copy(k, peer_of(k)).start()

    part_mid[0] = part_out[me]

    @pl.loop(n // 2, n)
    def _(k):
        send_pages(k)

    for s in range(SLOTS):
        page = ids_smem[0, 0, s]
        land_c[0, s] = cc[page]
        land_k[0, s] = kp[page]

    @pl.loop(0, n_blk)
    def _(col):
        total = jnp.zeros((CHUNK, W_BLK), F32)
        for r in range(n_row):
            w_copy(col, r).wait()
            total = total + jnp.dot(x_ref[:, r * W_ROWS:(r + 1) * W_ROWS], wbuf[r], preferred_element_type=F32)

            @pl.when(col + 1 < n_blk)
            def _():
                w_copy(col + 1, r).start()

        q_all[:, pl.ds(pl.multiple_of(col * W_BLK, W_BLK), W_BLK)] = total.astype(BF16)

    def h_copy(src, i, slot):
        return pltpu.make_async_copy(src.at[:, pl.ds(pl.multiple_of(i * H_BLK, H_BLK), H_BLK)], hbuf.at[slot], h_sem.at[slot])

    h_copy(w_uk, 0, 0).start()

    @pl.loop(0, n_h)
    def _(i):
        slot = i % 2
        h_copy(w_uk, i, slot).wait()

        @pl.when(i + 1 < n_h)
        def _():
            h_copy(w_uk, i + 1, 1 - slot).start()

        h32[...] = hbuf[slot].astype(F32)
        for pair in range(H_BLK // 2):
            q2 = q_all[:, pl.ds(pl.multiple_of((i * (H_BLK // 2) + pair) * 384, 128), 384)]
            q32 = q2.astype(F32)
            for odd in range(2):
                j = pair * 2 + odd
                base = odd * (NOPE_DIM + ROPE_DIM)
                wk = h32[:, j, :].astype(BF16)
                u = lax.dot_general(q2[:, base:base + NOPE_DIM], wk, LAST_DIMS, preferred_element_type=F32)
                qr = rope(q32[:, base + NOPE_DIM:base + NOPE_DIM + ROPE_DIM], cos2, sin2).astype(BF16)
                at = pl.ds(pl.multiple_of((i * H_BLK + j) * CHUNK, CHUNK), CHUNK)
                qc[at, :] = u.astype(BF16)
                qk[at, :] = jnp.concatenate([qr, qr], axis=-1)

    def ho_copy(i):
        return pltpu.make_async_copy(hout, wuv_out.at[pl.ds(pl.multiple_of(i * H_BLK, H_BLK), H_BLK)], ho_sem.at[0])

    h_copy(w_uv, 0, 0).start()

    @pl.loop(0, n_h)
    def _(i):
        slot = i % 2
        h_copy(w_uv, i, slot).wait()

        @pl.when(i + 1 < n_h)
        def _():
            h_copy(w_uv, i + 1, 1 - slot).start()

        h32[...] = hbuf[slot].astype(F32)

        @pl.when(i > 0)
        def _():
            ho_copy(i - 1).wait()

        for j in range(H_BLK):
            hout[j] = h32[:, j, :].astype(BF16)
        ho_copy(i).start()

    def tile(at, s, keys):
        m_old = m_ref[at, :]
        m_new = jnp.maximum(m_old, jnp.max(s, axis=-1, keepdims=True))
        alpha = jnp.exp2(m_old - m_new)
        groups = s.shape[1] // 128
        parts = [jnp.exp2(s[:, g * 128:(g + 1) * 128] - m_new) for g in range(groups)]
        total = parts[0]
        for p in parts[1:]:
            total = total + p
        m_ref[at, :] = m_new
        l_ref[at, :] = l_ref[at, :] * alpha + total
        p = jnp.concatenate([p.astype(BF16) for p in parts], axis=-1)
        pv = jnp.dot(p, keys, preferred_element_type=F32)
        for g in range(LATENT // 128):
            lanes = slice(g * 128, (g + 1) * 128)
            acc[at, lanes] = acc[at, lanes] * alpha + pv[:, lanes]

    first_lanes = lax.broadcasted_iota(jnp.int32, (CHUNK, 2 * ROPE_DIM), 1) < ROPE_DIM

    @pl.loop(0, ROWS // (SUB * SUBS))
    def _(i):
        causal = (lax.broadcasted_iota(jnp.int32, (SUB, CHUNK), 1) <= lax.broadcasted_iota(jnp.int32, (SUB, CHUNK), 0) % CHUNK)
        k64 = jnp.concatenate([new_k[...], jnp.zeros((CHUNK, ROPE_DIM), BF16)], axis=-1)
        ats = [pl.ds(pl.multiple_of((i * SUBS + u) * SUB, SUB), SUB) for u in range(SUBS)]
        raw = []
        for at in ats:
            s = lax.dot_general(qc[at, :], new_c[...], LAST_DIMS, preferred_element_type=F32)
            raw.append(s + lax.dot_general(qk[at, :], k64, LAST_DIMS, preferred_element_type=F32))
        for at, s in zip(ats, raw):
            s = jnp.where(causal, s * SCALE2, -jnp.inf)
            m = jnp.max(s, axis=-1, keepdims=True)
            p = jnp.exp2(s - m)
            m_ref[at, :] = jnp.broadcast_to(m, (SUB, 128))
            l_ref[at, :] = jnp.concatenate([p, jnp.zeros((SUB, 128 - CHUNK), F32)], axis=-1)
            acc[at, :] = jnp.dot(p.astype(BF16), new_c[...], preferred_element_type=F32)

    half_low = lax.broadcasted_iota(jnp.int32, (PAGE_LEN // 2, 2 * ROPE_DIM), 1) < ROPE_DIM

    @pl.loop(0, n // 2)
    def _(t):
        @pl.when(t > 0)
        def _():
            c_copy(2 * t, any_peer).wait_recv()
            k_copy(2 * t, any_peer).wait_recv()

        c_copy(2 * t + 1, any_peer).wait_recv()
        k_copy(2 * t + 1, any_peer).wait_recv()

        for d in range(2):
            for s in range(SLOTS):
                page = land_k[2 * t + d, s]
                zero = jnp.zeros_like(page)
                base = (d * SLOTS + s) * PAGE_LEN
                kk[base:base + PAGE_LEN // 2, :] = jnp.where(half_low, page, zero)
                kk[base + PAGE_LEN // 2:base + PAGE_LEN, :] = jnp.where(half_low, zero, page)

        @pl.loop(0, ROWS // (SUB * SUBS))
        def _(i):
            keys = land_c[pl.ds(2 * t, 2)].reshape(2 * SLOTS * PAGE_LEN, LATENT)
            bias = bias_ref[t]
            ats = [pl.ds(pl.multiple_of((i * SUBS + u) * SUB, SUB), SUB) for u in range(SUBS)]
            raw = []
            for at in ats:
                s = lax.dot_general(qc[at, :], keys, LAST_DIMS, preferred_element_type=F32)
                raw.append(s + lax.dot_general(qk[at, :], kk[...], LAST_DIMS, preferred_element_type=F32))
            for at, s in zip(ats, raw):
                tile(at, s * SCALE2 + bias, keys)

        @pl.when(t == n // 2 - 6)
        def _():
            @pl.loop(1, n)
            def _(k):
                p_copy(k, any_peer).wait_recv()

            @pl.loop(0, n)
            def _(k):
                owner = peer_of(k)
                source = jnp.int32(0)
                for j in range(n):
                    source = jnp.where(ids_smem[j, 0, SLOTS] == owner, j, source)
                part_fwd[k] = part_mid[source]

            @pl.loop(1, n)
            def _(k):
                f_copy(k, peer_of(k)).start()

            part_in[me] = part_fwd[0]

    @pl.loop(0, ROWS // SUB)
    def _(i):
        at = pl.ds(pl.multiple_of(i * SUB, SUB), SUB)
        share = 1.0 / jnp.sum(l_ref[at, :], axis=-1, keepdims=True)
        qc[at, :] = (acc[at, :] * share).astype(BF16)

    out = pltpu.make_async_copy(qc, o_lat, out_sem.at[0])
    out.start()

    @pl.loop(1, n)
    def _(k):
        f_copy(k, any_peer).wait_recv()

    for i in range(n):
        part = part_in[i].astype(F32)
        c32[2 * i, 0:4] = part[0:4]
        c32[2 * i + 1, 0:4] = part[4:8]
        c32[2 * i, 4:5] = part[8:9]
        c32[2 * i + 1, 4:5] = jnp.concatenate([part[8:9, ROPE_DIM:], part[8:9, :ROPE_DIM]], axis=-1)
    for g in range(LATENT // 128):
        new_c[:, g * 128:(g + 1) * 128] = c32[:, g, :].astype(BF16)
    new_k[...] = c32[:, 4, :][:, :ROPE_DIM].astype(BF16)
    out_pc = pltpu.make_async_copy(new_c, page_c_out, out_sem.at[1])
    out_pk = pltpu.make_async_copy(new_k, page_k_out, out_sem.at[2])
    out_pc.start()
    out_pk.start()

    @pl.loop(1, n)
    def _(k):
        id_copy(k, any_peer).wait_send()
        c_copy(k, any_peer).wait_send()
        k_copy(k, any_peer).wait_send()
        p_copy(k, any_peer).wait_send()
        f_copy(k, any_peer).wait_send()

    ho_copy(n_h - 1).wait()
    out.wait()
    out_pc.wait()
    out_pk.wait()


def layer(n, ids, x, bias, rot, gain, cache_c, cache_kr, w_q, w_dkv, w_uk, w_uv):
    pages = cache_c.shape[0] - 1
    any_spec = pl.BlockSpec(memory_space=pl.ANY)
    vmem = pl.BlockSpec(memory_space=pltpu.VMEM)
    dma = pltpu.SemaphoreType.DMA
    return pl.pallas_call(
        functools.partial(layer_kernel, n),
        name="layer",
        out_shape=(
            jax.ShapeDtypeStruct((ROWS, LATENT), BF16),
            jax.ShapeDtypeStruct((HEADS, LATENT, VALUE_DIM), BF16),
            jax.ShapeDtypeStruct((CHUNK, LATENT), BF16),
            jax.ShapeDtypeStruct((CHUNK, ROPE_DIM), BF16),
        ),
        in_specs=[vmem] * 5 + [any_spec] * 6,
        out_specs=(any_spec,) * 4,
        scratch_shapes=[
            pltpu.VMEM((n, 1, 128), jnp.int32),
            pltpu.SMEM((n, 1, 128), jnp.int32),
            pltpu.VMEM((pages, PAGE_LEN, LATENT), BF16),
            pltpu.VMEM((pages, PAGE_LEN, ROPE_DIM), BF16),
            pltpu.VMEM((pages, PAGE_LEN // 2, 2 * ROPE_DIM), BF16),
            pltpu.VMEM((n, SLOTS, PAGE_LEN, LATENT), BF16),
            pltpu.VMEM((n, SLOTS, PAGE_LEN // 2, 2 * ROPE_DIM), BF16),
            pltpu.VMEM((n, SLOTS, PAGE_LEN, LATENT), BF16),
            pltpu.VMEM((n, SLOTS, PAGE_LEN // 2, 2 * ROPE_DIM), BF16),
            pltpu.VMEM((W_BUFS, W_ROWS, W_BLK), BF16),
            pltpu.VMEM((CHUNK, HEADS * (NOPE_DIM + ROPE_DIM)), BF16),
            pltpu.VMEM((ROWS, LATENT), BF16),
            pltpu.VMEM((ROWS, 2 * ROPE_DIM), BF16),
            pltpu.VMEM((ROWS, 128), F32),
            pltpu.VMEM((ROWS, 128), F32),
            pltpu.VMEM((ROWS, LATENT), F32),
            pltpu.VMEM((2, LATENT, H_BLK, NOPE_DIM), BF16),
            pltpu.VMEM((LATENT, H_BLK, NOPE_DIM), F32),
            pltpu.VMEM((H_BLK, LATENT, VALUE_DIM), BF16),
            pltpu.VMEM((2, LATENT + ROPE_DIM, KV_ROWS), BF16),
            pltpu.VMEM((CHUNK, LATENT), BF16),
            pltpu.VMEM((CHUNK, ROPE_DIM), BF16),
            pltpu.VMEM((2 * SLOTS * PAGE_LEN, 2 * ROPE_DIM), BF16),
            pltpu.VMEM((n, 16, 128), BF16),
            pltpu.VMEM((n, 16, 128), BF16),
            pltpu.VMEM((n, 16, 128), BF16),
            pltpu.VMEM((n, 16, 128), BF16),
            pltpu.VMEM((CHUNK, 8, 128), F32),
            dma((4,)),
        ] + [dma((n,))] * 10 + [dma((W_BUFS,)), dma((2,)), dma((1,)), dma((2,)), dma((3,))],
        compiler_params=pltpu.CompilerParams(collective_id=0, has_side_effects=True, vmem_limit_bytes=VMEM_LIMIT),
    )(ids, x, bias, rot, gain, cache_c, cache_kr, w_q, w_dkv, w_uk, w_uv)


O_BLK = 256
O_BUFS = 6


def finish_kernel(x_ref, o_lat, wuv, w_o, cache_c, cache_kr, page_c, page_k, y_ref, out_c, out_kr,
                  lat, wv, heads, wbuf, cbuf, kbuf, lat_sem, wv_sem, w_sem, in_sem, out_sem):
    n_blk = w_o.shape[1] // O_BLK
    n_h = HEADS // H_BLK
    pages = cache_c.shape[0] - 1

    def lat_copy(i):
        at = pl.ds(pl.multiple_of(i * H_BLK * CHUNK, 8), H_BLK * CHUNK)
        return pltpu.make_async_copy(o_lat.at[at], lat.at[at], lat_sem.at[i])

    def wv_copy(i):
        at = pl.ds(pl.multiple_of(i * H_BLK, H_BLK), H_BLK)
        return pltpu.make_async_copy(wuv.at[at], wv.at[at], wv_sem.at[i])

    def w_copy(i, slot):
        return pltpu.make_async_copy(w_o.at[:, pl.ds(pl.multiple_of(i * O_BLK, O_BLK), O_BLK)], wbuf.at[slot], w_sem.at[slot])

    for i in range(n_h):
        lat_copy(i).start()
        wv_copy(i).start()
    ins = [pltpu.make_async_copy(cache_c.at[pl.ds(0, pages)], cbuf.at[pl.ds(0, pages)], in_sem.at[0]),
           pltpu.make_async_copy(cache_kr.at[pl.ds(0, pages)], kbuf.at[pl.ds(0, pages)], in_sem.at[1]),
           pltpu.make_async_copy(page_c, cbuf.at[pages], in_sem.at[2]),
           pltpu.make_async_copy(page_k, kbuf.at[pages], in_sem.at[3])]
    for i in range(O_BUFS):
        w_copy(i, i).start()
    for c in ins:
        c.start()

    @pl.loop(0, n_h)
    def _(i):
        lat_copy(i).wait()
        wv_copy(i).wait()
        for j in range(H_BLK):
            h = i * H_BLK + j
            o = jnp.dot(lat[pl.ds(pl.multiple_of(h * CHUNK, CHUNK), CHUNK), :], wv[h], preferred_element_type=F32)
            heads[:, pl.ds(pl.multiple_of(h * VALUE_DIM, VALUE_DIM), VALUE_DIM)] = o.astype(BF16)

    for c in ins:
        c.wait()
    outs = [pltpu.make_async_copy(cbuf, out_c, out_sem.at[0]), pltpu.make_async_copy(kbuf, out_kr, out_sem.at[1])]
    for c in outs:
        c.start()

    @pl.loop(0, n_blk)
    def _(i):
        slot = lax.rem(i, O_BUFS)
        w_copy(i, slot).wait()
        at = pl.ds(pl.multiple_of(i * O_BLK, O_BLK), O_BLK)
        part = jnp.dot(heads[...], wbuf[slot], preferred_element_type=F32)
        y_ref[:, at] = (x_ref[:, at].astype(F32) + part).astype(BF16)

        @pl.when(i + O_BUFS < n_blk)
        def _():
            w_copy(i + O_BUFS, slot).start()

    for c in outs:
        c.wait()


def finish(x, o_lat, wuv, w_o, cache_c, cache_kr, page_c, page_k):
    any_spec = pl.BlockSpec(memory_space=pl.ANY)
    vmem = pl.BlockSpec(memory_space=pltpu.VMEM)
    dma = pltpu.SemaphoreType.DMA
    n_h = HEADS // H_BLK
    return pl.pallas_call(
        finish_kernel,
        name="finish",
        out_shape=(
            jax.ShapeDtypeStruct(x.shape, BF16),
            jax.ShapeDtypeStruct(cache_c.shape, BF16),
            jax.ShapeDtypeStruct(cache_kr.shape, BF16),
        ),
        in_specs=[vmem] + [any_spec] * 7,
        out_specs=(vmem, any_spec, any_spec),
        scratch_shapes=[
            pltpu.VMEM(o_lat.shape, BF16),
            pltpu.VMEM(wuv.shape, BF16),
            pltpu.VMEM((CHUNK, HEADS * VALUE_DIM), BF16),
            pltpu.VMEM((O_BUFS, HEADS * VALUE_DIM, O_BLK), BF16),
            pltpu.VMEM(cache_c.shape, BF16),
            pltpu.VMEM(cache_kr.shape, BF16),
            dma((n_h,)),
            dma((n_h,)),
            dma((O_BUFS,)),
            dma((4,)),
            dma((2,)),
        ],
        compiler_params=pltpu.CompilerParams(vmem_limit_bytes=VMEM_LIMIT),
    )(x, o_lat, wuv, w_o, cache_c, cache_kr, page_c, page_k)


def solution(mesh):
    n = mesh.shape["pool"]

    def device_step(hidden, pre_len, pre_table, wr_table, cache_c, cache_kr, w_q, w_dkv, g_kv, w_uk, w_uv, w_o):
        x = hidden[0]
        me = lax.axis_index("pool")
        owners = pre_table[0, :, 0]
        table_pages = owners.shape[0]
        earlier = jnp.arange(table_pages)[:, None] > jnp.arange(table_pages)[None, :]
        rank = jnp.sum(jnp.where(earlier & (owners[:, None] == owners[None, :]), 1, 0), axis=1)
        pos = jnp.where(owners >= 0, owners * SLOTS + rank, -1)
        lanes = jnp.arange(128, dtype=jnp.int32)
        slot_of = jnp.where(lanes < SLOTS, jnp.arange(n, dtype=jnp.int32)[:, None] * SLOTS + lanes, -2)
        asked = jnp.sum(jnp.where(pos[None, None, :] == slot_of[:, :, None], pre_table[0, :, 1], 0), axis=2)
        ids = jnp.where(lanes == SLOTS, wr_table[0, 0, 0], asked)[:, None, :].astype(jnp.int32)
        keys = jnp.arange(2 * SLOTS * PAGE_LEN, dtype=jnp.int32)
        owner_of = jnp.bitwise_xor(me, jnp.arange(n // 2, dtype=jnp.int32)[:, None] + 16 * (keys // (SLOTS * PAGE_LEN)))
        counts = jnp.sum(jnp.where(owner_of[:, :: SLOTS * PAGE_LEN, None] == owners, 1, 0), axis=2)
        counts = jnp.repeat(counts, SLOTS * PAGE_LEN, axis=1)
        bias = jnp.where((keys // PAGE_LEN) % SLOTS < counts, 0.0, -jnp.inf).astype(F32)[:, None, :]
        cos_tab, sin_tab = rope_tables(pre_len[0] + jnp.arange(CHUNK))
        rot = jnp.stack([jnp.concatenate([cos_tab, cos_tab], -1), jnp.concatenate([-sin_tab, sin_tab], -1)])
        o_lat, wuv, page_c, page_k = layer(n, ids, x, bias, rot, g_kv.astype(F32)[None], cache_c[0], cache_kr[0], w_q, w_dkv.T, w_uk, w_uv)
        y, out_c, out_kr = finish(x, o_lat, wuv, w_o, cache_c[0], cache_kr[0], page_c, page_k)
        return y[None], out_c[None], out_kr[None]

    row_spec = P("pool")
    rep_spec = P()
    return jax.shard_map(device_step, mesh=mesh, in_specs=(row_spec,) * 6 + (rep_spec,) * 6, out_specs=(row_spec,) * 3, check_vma=False)


def rope_tables(positions):
    half_dim = ROPE_DIM // 2
    inv_freq = ROPE_BASE ** (-jnp.arange(half_dim, dtype=F32) / half_dim)
    angles = positions.astype(F32)[..., None] * inv_freq
    return jnp.cos(angles), jnp.sin(angles)
```

```python
import functools

import jax
import jax.numpy as jnp
from jax import lax
from jax.experimental import pallas as pl
from jax.experimental.pallas import tpu as pltpu
from jax.sharding import PartitionSpec as P

PAGE_LEN = 64
LATENT = 512
ROPE_DIM = 64
NOPE_DIM = 128
VALUE_DIM = 128
HEADS = 64
CHUNK = 64
D_MODEL = 7168
SLOTS = 4
NORM_EPS = 1e-6
ROPE_BASE = 10000.0
MESH = pl.DeviceIdType.MESH
VMEM_LIMIT = 63 * 1024 * 1024
SCALE2 = (NOPE_DIM + ROPE_DIM) ** -0.5 * 1.4426950408889634
ROWS = HEADS * CHUNK
SUB = 256
SUBS = 4
W_BLK = 512
W_ROWS = 1792
W_BUFS = 4
KV_ROWS = 512
H_BLK = 8
CORE_HEADS = HEADS // 2
HALF = CORE_HEADS * CHUNK
RING = 3
LAST_DIMS = (((1,), (1,)), ((), ()))
BF16 = jnp.bfloat16
F32 = jnp.float32


def step_code(k):
    return lax.div(k, 2) + 16 * lax.rem(k, 2)


def flip_weights(me, bits):
    return [2 ** i - 2 ** (i + 1) * lax.rem(lax.div(me, 2 ** i), 2) for i in range(bits)]


def flipped(me, flips, code):
    out = me
    for i, f in enumerate(flips):
        out = out + f * lax.rem(lax.div(code, 2 ** i), 2)
    return out


def rope(values, cos2, sin2):
    half = ROPE_DIM // 2
    swapped = jnp.concatenate([values[:, half:], values[:, :half]], axis=-1)
    return values * cos2 + swapped * sin2


def layer_kernel(n, ids_ref, bias_ref, rot_ref, gain_ref, x_ref, cache_c, cache_kr, w_q, w_dkv, w_uk, w_uv,
                 o_lat, wuv_out, page_c_out, page_k_out,
                 ids_in, ids_smem, cc, ck, kp, stage_c, stage_k, land_c, land_k, ring_c, ring_k, wbuf, q_all, qc, qk, m_ref, l_ref, acc,
                 hbuf, h32, hout, kvbuf, xb, bias_p, rot_p, new_c, new_k, kk, part_out, part_mid, part_fwd, part_in, c32,
                 loc_sem, id_send, id_recv, c_send, c_recv, k_send, k_recv, p_send, p_recv, f_send, f_recv, w_sem, h_sem, ho_sem, kv_sem, out_sem,
                 pair_send, pair_recv, rc_send, rc_recv, rk_send, rk_recv, credit):
    me = lax.axis_index("pool")
    bits = n.bit_length() - 1
    pages = kp.shape[0]
    core = lax.rem(me, 2)
    n_blk = w_q.shape[1] // 2 // W_BLK
    n_kv = D_MODEL // KV_ROWS
    n_h = CORE_HEADS // H_BLK

    load_c = pltpu.make_async_copy(cache_c.at[pl.ds(0, pages)], cc, loc_sem.at[0])
    load_k = pltpu.make_async_copy(cache_kr.at[pl.ds(0, pages)], ck, loc_sem.at[1])
    load_k.start()
    load_c.start()

    flips = flip_weights(me, bits)
    any_peer = lax.rem(me + 1, n)
    partner = me + flips[0]

    def peer_of(k):
        return flipped(me, flips, step_code(k))

    barrier = pltpu.get_barrier_semaphore()

    @pl.loop(1, n)
    def _(k):
        pl.semaphore_signal(barrier, inc=1, device_id=(peer_of(k),), device_id_type=MESH)

    def kv_copy(i, slot):
        return pltpu.make_async_copy(w_dkv.at[:, pl.ds(i * KV_ROWS, KV_ROWS)], kvbuf.at[slot], kv_sem.at[slot])

    n_row = D_MODEL // W_ROWS

    def w_copy(col, r):
        rows = pl.ds(r * W_ROWS, W_ROWS)
        return pltpu.make_async_copy(w_q.at[rows, pl.ds(pl.multiple_of((core * n_blk + col) * W_BLK, W_BLK), W_BLK)], wbuf.at[r], w_sem.at[r])

    kv_copy(0, 0).start()
    kv_copy(1, 1).start()
    own_x = pltpu.make_async_copy(x_ref, xb.at[pl.ds(0, CHUNK)], loc_sem.at[4])
    own_x.start()
    pl.semaphore_wait(barrier, n - 1)

    def pair_copy(i, src, dst):
        return pltpu.make_async_remote_copy(src_ref=src, dst_ref=dst, send_sem=pair_send.at[i], recv_sem=pair_recv.at[i],
                                            device_id=(partner,), device_id_type=MESH)

    pair = [pair_copy(0, x_ref, xb.at[pl.ds(CHUNK, CHUNK)]), pair_copy(1, rot_ref, rot_p), pair_copy(2, bias_ref, bias_p)]

    def id_copy(k, peer):
        return pltpu.make_async_remote_copy(src_ref=ids_ref.at[peer], dst_ref=ids_in.at[k], send_sem=id_send.at[k],
                                            recv_sem=id_recv.at[k], device_id=(peer,), device_id_type=MESH)

    @pl.loop(1, n)
    def _(k):
        id_copy(k, peer_of(k)).start()

    own_ids = pltpu.make_async_copy(ids_ref.at[me], ids_in.at[0], loc_sem.at[2])
    own_ids.start()
    for c in pair:
        c.start()
    load_k.wait()

    @pl.loop(0, pages)
    def _(i):
        page = ck[i]
        kp[i] = jnp.concatenate([page[: PAGE_LEN // 2], page[PAGE_LEN // 2:]], axis=-1)

    load_c.wait()
    own_ids.wait()

    @pl.loop(1, n)
    def _(k):
        id_copy(k, any_peer).wait_recv()

    to_smem = pltpu.make_async_copy(ids_in, ids_smem, loc_sem.at[3])
    to_smem.start()
    to_smem.wait()

    def c_copy(k, peer):
        return pltpu.make_async_remote_copy(src_ref=stage_c.at[k], dst_ref=land_c.at[k], send_sem=c_send.at[k],
                                            recv_sem=c_recv.at[k], device_id=(peer,), device_id_type=MESH)

    def k_copy(k, peer):
        return pltpu.make_async_remote_copy(src_ref=stage_k.at[k], dst_ref=land_k.at[k], send_sem=k_send.at[k],
                                            recv_sem=k_recv.at[k], device_id=(peer,), device_id_type=MESH)

    def launch(k):
        peer = peer_of(k)
        c_copy(k, peer).start()
        k_copy(k, peer).start()

    def send_pages(k, first):
        for s in range(SLOTS):
            page = ids_smem[k, 0, s]
            stage_c[k, s] = cc[page]
            stage_k[k, s] = kp[page]

        @pl.when(k > first)
        def _():
            launch(k - 1)

    @pl.loop(1, n // 2)
    def _(k):
        send_pages(k, 1)

    launch(n // 2 - 1)

    for r in range(n_row):
        w_copy(0, r).start()

    own_x.wait()
    for c in pair:
        c.wait_recv()
    kv = jnp.zeros((2 * CHUNK, LATENT + ROPE_DIM), F32)
    for i in range(n_kv):
        kv_copy(i, i % 2).wait()
        kv = kv + lax.dot_general(xb[:, i * KV_ROWS:(i + 1) * KV_ROWS], kvbuf[i % 2], LAST_DIMS, preferred_element_type=F32)
        if i + 2 < n_kv:
            kv_copy(i + 2, i % 2).start()
    lat = kv[:, :LATENT]
    inv_rms = lax.rsqrt(jnp.mean(lat * lat, axis=-1, keepdims=True) + NORM_EPS)
    c_new = (lat * inv_rms * gain_ref[...]).astype(BF16)
    cos2 = jnp.concatenate([rot_ref[0], rot_p[0]], axis=0)
    sin2 = jnp.concatenate([rot_ref[1], rot_p[1]], axis=0)
    kr_new = rope(kv[:, LATENT:], cos2, sin2).astype(BF16)
    new_c[...] = c_new
    new_k[...] = kr_new

    for g in range(LATENT // 128):
        c32[:, g, :] = c_new[:CHUNK, g * 128:(g + 1) * 128].astype(F32)
    c32[:, 4, :] = jnp.concatenate([kr_new[:CHUNK], kr_new[:CHUNK]], axis=-1).astype(F32)
    low = lax.broadcasted_iota(jnp.int32, (1, 128), 1) < ROPE_DIM
    for i in range(n):
        a = c32[2 * i]
        b = c32[2 * i + 1]
        last = jnp.where(low, a[4:5], b[4:5])
        part_out[i] = jnp.concatenate([a[:4], b[:4], jnp.broadcast_to(last, (8, 128))], axis=0).astype(BF16)

    def p_copy(k, peer):
        return pltpu.make_async_remote_copy(src_ref=part_out.at[peer], dst_ref=part_mid.at[k], send_sem=p_send.at[k],
                                            recv_sem=p_recv.at[k], device_id=(peer,), device_id_type=MESH)

    def f_copy(k, peer):
        return pltpu.make_async_remote_copy(src_ref=part_fwd.at[k], dst_ref=part_in.at[me], send_sem=f_send.at[k],
                                            recv_sem=f_recv.at[k], device_id=(peer,), device_id_type=MESH)

    @pl.loop(1, n)
    def _(k):
        p_copy(k, peer_of(k)).start()

    part_mid[0] = part_out[me]

    @pl.loop(n // 2, n)
    def _(k):
        send_pages(k, n // 2)

    for s in range(SLOTS):
        page = ids_smem[0, 0, s]
        land_c[0, s] = cc[page]
        land_k[0, s] = kp[page]
    launch(n - 1)

    @pl.loop(0, n_blk)
    def _(col):
        total = jnp.zeros((2 * CHUNK, W_BLK), F32)
        for r in range(n_row):
            w_copy(col, r).wait()
            total = total + jnp.dot(xb[:, r * W_ROWS:(r + 1) * W_ROWS], wbuf[r], preferred_element_type=F32)

            @pl.when(col + 1 < n_blk)
            def _():
                w_copy(col + 1, r).start()

        q_all[:, pl.ds(pl.multiple_of(col * W_BLK, W_BLK), W_BLK)] = total.astype(BF16)

    def h_copy(src, i, slot):
        return pltpu.make_async_copy(src.at[:, pl.ds(pl.multiple_of(core * CORE_HEADS + i * H_BLK, H_BLK), H_BLK)], hbuf.at[slot], h_sem.at[slot])

    h_copy(w_uk, 0, 0).start()

    @pl.loop(0, n_h)
    def _(i):
        slot = i % 2
        h_copy(w_uk, i, slot).wait()

        @pl.when(i + 1 < n_h)
        def _():
            h_copy(w_uk, i + 1, 1 - slot).start()

        h32[...] = hbuf[slot].astype(F32)
        for pair in range(H_BLK // 2):
            q2 = q_all[:, pl.ds(pl.multiple_of((i * (H_BLK // 2) + pair) * 384, 128), 384)]
            q32 = q2.astype(F32)
            for odd in range(2):
                j = pair * 2 + odd
                base = odd * (NOPE_DIM + ROPE_DIM)
                wk = h32[:, j, :].astype(BF16)
                u = lax.dot_general(q2[:, base:base + NOPE_DIM], wk, LAST_DIMS, preferred_element_type=F32)
                qr = rope(q32[:, base + NOPE_DIM:base + NOPE_DIM + ROPE_DIM], cos2, sin2).astype(BF16)
                at = pl.ds(pl.multiple_of((i * H_BLK + j) * CHUNK, CHUNK), CHUNK)
                far = pl.ds(pl.multiple_of((CORE_HEADS + i * H_BLK + j) * CHUNK, CHUNK), CHUNK)
                qc[at, :] = u[:CHUNK].astype(BF16)
                qc[far, :] = u[CHUNK:].astype(BF16)
                twice = jnp.concatenate([qr, qr], axis=-1)
                qk[at, :] = twice[:CHUNK]
                qk[far, :] = twice[CHUNK:]

    def ho_copy(i):
        return pltpu.make_async_copy(hout, wuv_out.at[pl.ds(pl.multiple_of(i * H_BLK, H_BLK), H_BLK)], ho_sem.at[0])

    h_copy(w_uv, 0, 0).start()

    @pl.loop(0, n_h)
    def _(i):
        slot = i % 2
        h_copy(w_uv, i, slot).wait()

        @pl.when(i + 1 < n_h)
        def _():
            h_copy(w_uv, i + 1, 1 - slot).start()

        h32[...] = hbuf[slot].astype(F32)

        @pl.when(i > 0)
        def _():
            ho_copy(i - 1).wait()

        for j in range(H_BLK):
            hout[j] = h32[:, j, :].astype(BF16)
        ho_copy(i).start()

    def tile(at, s, keys):
        m_old = m_ref[at, :]
        m_new = jnp.maximum(m_old, jnp.max(s, axis=-1, keepdims=True))
        alpha = jnp.exp2(m_old - m_new)
        groups = s.shape[1] // 128
        parts = [jnp.exp2(s[:, g * 128:(g + 1) * 128] - m_new) for g in range(groups)]
        total = parts[0]
        for p in parts[1:]:
            total = total + p
        m_ref[at, :] = m_new
        l_ref[at, :] = l_ref[at, :] * alpha + total
        p = jnp.concatenate([p.astype(BF16) for p in parts], axis=-1)
        pv = jnp.dot(p, keys, preferred_element_type=F32)
        for g in range(LATENT // 128):
            lanes = slice(g * 128, (g + 1) * 128)
            acc[at, lanes] = acc[at, lanes] * alpha + pv[:, lanes]

    def row_tiles(half, i):
        return [pl.ds(pl.multiple_of(half * HALF + (i * SUBS + u) * SUB, SUB), SUB) for u in range(SUBS)]

    for half in range(2):
        @pl.loop(0, HALF // (SUB * SUBS))
        def _(i):
            causal = (lax.broadcasted_iota(jnp.int32, (SUB, CHUNK), 1) <= lax.broadcasted_iota(jnp.int32, (SUB, CHUNK), 0) % CHUNK)
            c64 = new_c[half * CHUNK:(half + 1) * CHUNK, :]
            k64 = jnp.concatenate([new_k[half * CHUNK:(half + 1) * CHUNK, :], jnp.zeros((CHUNK, ROPE_DIM), BF16)], axis=-1)
            ats = row_tiles(half, i)
            raw = []
            for at in ats:
                s = lax.dot_general(qc[at, :], c64, LAST_DIMS, preferred_element_type=F32)
                raw.append(s + lax.dot_general(qk[at, :], k64, LAST_DIMS, preferred_element_type=F32))
            for at, s in zip(ats, raw):
                s = jnp.where(causal, s * SCALE2, -jnp.inf)
                m = jnp.max(s, axis=-1, keepdims=True)
                p = jnp.exp2(s - m)
                m_ref[at, :] = jnp.broadcast_to(m, (SUB, 128))
                l_ref[at, :] = jnp.concatenate([p, jnp.zeros((SUB, 128 - CHUNK), F32)], axis=-1)
                acc[at, :] = jnp.dot(p.astype(BF16), c64, preferred_element_type=F32)

    half_low = lax.broadcasted_iota(jnp.int32, (PAGE_LEN // 2, 2 * ROPE_DIM), 1) < ROPE_DIM

    def spread(page_of):
        for d in range(2):
            for s in range(SLOTS):
                page = page_of(d, s)
                zero = jnp.zeros_like(page)
                base = (d * SLOTS + s) * PAGE_LEN
                kk[base:base + PAGE_LEN // 2, :] = jnp.where(half_low, page, zero)
                kk[base + PAGE_LEN // 2:base + PAGE_LEN, :] = jnp.where(half_low, zero, page)

    def attend(half, keys_of, bias_of):
        @pl.loop(0, HALF // (SUB * SUBS))
        def _(i):
            keys = keys_of().reshape(2 * SLOTS * PAGE_LEN, LATENT)
            bias = bias_of()
            ats = row_tiles(half, i)
            raw = []
            for at in ats:
                s = lax.dot_general(qc[at, :], keys, LAST_DIMS, preferred_element_type=F32)
                raw.append(s + lax.dot_general(qk[at, :], kk[...], LAST_DIMS, preferred_element_type=F32))
            for at, s in zip(ats, raw):
                tile(at, s * SCALE2 + bias, keys)

    steps = n // 2

    def ring_copies(t):
        r = lax.rem(t, RING)
        return (pltpu.make_async_remote_copy(src_ref=land_c.at[pl.ds(2 * t, 2)], dst_ref=ring_c.at[r], send_sem=rc_send.at[r],
                                             recv_sem=rc_recv.at[r], device_id=(partner,), device_id_type=MESH),
                pltpu.make_async_remote_copy(src_ref=land_k.at[pl.ds(2 * t, 2)], dst_ref=ring_k.at[r], send_sem=rk_send.at[r],
                                             recv_sem=rk_recv.at[r], device_id=(partner,), device_id_type=MESH))

    @pl.loop(0, steps + 1)
    def _(t):
        @pl.when(t < steps)
        def _():
            @pl.when(t > 0)
            def _():
                c_copy(2 * t, any_peer).wait_recv()
                k_copy(2 * t, any_peer).wait_recv()

            c_copy(2 * t + 1, any_peer).wait_recv()
            k_copy(2 * t + 1, any_peer).wait_recv()

            @pl.when(t >= RING)
            def _():
                for c in ring_copies(t - RING):
                    c.wait_send()
                pl.semaphore_wait(credit, 1)

            for c in ring_copies(t):
                c.start()
            spread(lambda d, s: land_k[2 * t + d, s])
            attend(0, lambda: land_c[pl.ds(2 * t, 2)], lambda: bias_ref[t])

        @pl.when(t > 0)
        def _():
            r = lax.rem(t - 1, RING)
            for c in ring_copies(t - 1):
                c.wait_recv()
            spread(lambda d, s: ring_k[r, d, s])
            attend(1, lambda: ring_c[r], lambda: bias_p[t - 1])

            @pl.when(t - 1 < steps - RING)
            def _():
                pl.semaphore_signal(credit, inc=1, device_id=(partner,), device_id_type=MESH)

        @pl.when(t == n // 2 - 6)
        def _():
            @pl.loop(1, n)
            def _(k):
                p_copy(k, any_peer).wait_recv()

            @pl.loop(0, n)
            def _(k):
                owner = peer_of(k)
                source = jnp.int32(0)
                for j in range(n):
                    source = jnp.where(ids_smem[j, 0, SLOTS] == owner, j, source)
                part_fwd[k] = part_mid[source]

            @pl.loop(1, n)
            def _(k):
                f_copy(k, peer_of(k)).start()

            part_in[me] = part_fwd[0]

    @pl.loop(0, ROWS // SUB)
    def _(i):
        at = pl.ds(pl.multiple_of(i * SUB, SUB), SUB)
        share = 1.0 / jnp.sum(l_ref[at, :], axis=-1, keepdims=True)
        qc[at, :] = (acc[at, :] * share).astype(BF16)

    out = pltpu.make_async_copy(qc, o_lat, out_sem.at[0])
    out.start()

    @pl.loop(1, n)
    def _(k):
        f_copy(k, any_peer).wait_recv()

    for i in range(n):
        part = part_in[i].astype(F32)
        c32[2 * i, 0:4] = part[0:4]
        c32[2 * i + 1, 0:4] = part[4:8]
        c32[2 * i, 4:5] = part[8:9]
        c32[2 * i + 1, 4:5] = jnp.concatenate([part[8:9, ROPE_DIM:], part[8:9, :ROPE_DIM]], axis=-1)
    for g in range(LATENT // 128):
        new_c[:CHUNK, g * 128:(g + 1) * 128] = c32[:, g, :].astype(BF16)
    new_k[:CHUNK, :] = c32[:, 4, :][:, :ROPE_DIM].astype(BF16)
    out_pc = pltpu.make_async_copy(new_c.at[pl.ds(0, CHUNK)], page_c_out, out_sem.at[1])
    out_pk = pltpu.make_async_copy(new_k.at[pl.ds(0, CHUNK)], page_k_out, out_sem.at[2])
    out_pc.start()
    out_pk.start()

    @pl.loop(1, n)
    def _(k):
        id_copy(k, any_peer).wait_send()
        c_copy(k, any_peer).wait_send()
        k_copy(k, any_peer).wait_send()
        p_copy(k, any_peer).wait_send()
        f_copy(k, any_peer).wait_send()

    for c in pair:
        c.wait_send()
    for t in range(steps - RING, steps):
        for c in ring_copies(t):
            c.wait_send()
    ho_copy(n_h - 1).wait()
    out.wait()
    out_pc.wait()
    out_pk.wait()


def layer(n, ids, bias, rot, gain, x, cache_c, cache_kr, w_q, w_dkv, w_uk, w_uv):
    pages = cache_c.shape[0] - 1
    any_spec = pl.BlockSpec(memory_space=pl.ANY)
    vmem = pl.BlockSpec(memory_space=pltpu.VMEM)
    dma = pltpu.SemaphoreType.DMA
    return pl.pallas_call(
        functools.partial(layer_kernel, n),
        name="layer",
        out_shape=(
            jax.ShapeDtypeStruct((ROWS, LATENT), BF16),
            jax.ShapeDtypeStruct((CORE_HEADS, LATENT, VALUE_DIM), BF16),
            jax.ShapeDtypeStruct((CHUNK, LATENT), BF16),
            jax.ShapeDtypeStruct((CHUNK, ROPE_DIM), BF16),
        ),
        in_specs=[vmem] * 4 + [any_spec] * 7,
        out_specs=(any_spec,) * 4,
        scratch_shapes=[
            pltpu.VMEM((n, 1, 128), jnp.int32),
            pltpu.SMEM((n, 1, 128), jnp.int32),
            pltpu.VMEM((pages, PAGE_LEN, LATENT), BF16),
            pltpu.VMEM((pages, PAGE_LEN, ROPE_DIM), BF16),
            pltpu.VMEM((pages, PAGE_LEN // 2, 2 * ROPE_DIM), BF16),
            pltpu.VMEM((n, SLOTS, PAGE_LEN, LATENT), BF16),
            pltpu.VMEM((n, SLOTS, PAGE_LEN // 2, 2 * ROPE_DIM), BF16),
            pltpu.VMEM((n, SLOTS, PAGE_LEN, LATENT), BF16),
            pltpu.VMEM((n, SLOTS, PAGE_LEN // 2, 2 * ROPE_DIM), BF16),
            pltpu.VMEM((RING, 2, SLOTS, PAGE_LEN, LATENT), BF16),
            pltpu.VMEM((RING, 2, SLOTS, PAGE_LEN // 2, 2 * ROPE_DIM), BF16),
            pltpu.VMEM((W_BUFS, W_ROWS, W_BLK), BF16),
            pltpu.VMEM((2 * CHUNK, CORE_HEADS * (NOPE_DIM + ROPE_DIM)), BF16),
            pltpu.VMEM((ROWS, LATENT), BF16),
            pltpu.VMEM((ROWS, 2 * ROPE_DIM), BF16),
            pltpu.VMEM((ROWS, 128), F32),
            pltpu.VMEM((ROWS, 128), F32),
            pltpu.VMEM((ROWS, LATENT), F32),
            pltpu.VMEM((2, LATENT, H_BLK, NOPE_DIM), BF16),
            pltpu.VMEM((LATENT, H_BLK, NOPE_DIM), F32),
            pltpu.VMEM((H_BLK, LATENT, VALUE_DIM), BF16),
            pltpu.VMEM((2, LATENT + ROPE_DIM, KV_ROWS), BF16),
            pltpu.VMEM((2 * CHUNK, D_MODEL), BF16),
            pltpu.VMEM(bias.shape, F32),
            pltpu.VMEM(rot.shape, F32),
            pltpu.VMEM((2 * CHUNK, LATENT), BF16),
            pltpu.VMEM((2 * CHUNK, ROPE_DIM), BF16),
            pltpu.VMEM((2 * SLOTS * PAGE_LEN, 2 * ROPE_DIM), BF16),
            pltpu.VMEM((n, 16, 128), BF16),
            pltpu.VMEM((n, 16, 128), BF16),
            pltpu.VMEM((n, 16, 128), BF16),
            pltpu.VMEM((n, 16, 128), BF16),
            pltpu.VMEM((CHUNK, 8, 128), F32),
            dma((5,)),
        ] + [dma((n,))] * 10 + [dma((W_BUFS,)), dma((2,)), dma((1,)), dma((2,)), dma((3,)), dma((3,)), dma((3,))] + [dma((RING,))] * 4 + [pltpu.SemaphoreType.REGULAR],
        compiler_params=pltpu.CompilerParams(collective_id=0, has_side_effects=True, vmem_limit_bytes=VMEM_LIMIT),
    )(ids, bias, rot, gain, x, cache_c, cache_kr, w_q, w_dkv, w_uk, w_uv)


O_BLK = 512
O_BUFS = 7


def finish_kernel(x_ref, o_lat, wuv, w_o, y_ref, lat, wv, heads, wbuf, own, going, coming, lat_sem, wv_sem, w_sem, s_send, s_recv):
    me = lax.axis_index("pool")
    core = lax.rem(me, 2)
    partner = me + 1 - 2 * core
    depth = CORE_HEADS * VALUE_DIM
    n_blk = w_o.shape[1] // O_BLK
    n_h = CORE_HEADS // H_BLK

    def lat_copy(half, i):
        at = pl.ds(pl.multiple_of(half * HALF + i * H_BLK * CHUNK, 8), H_BLK * CHUNK)
        return pltpu.make_async_copy(o_lat.at[at], lat.at[at], lat_sem.at[half, i])

    def wv_copy(i):
        at = pl.ds(pl.multiple_of(i * H_BLK, H_BLK), H_BLK)
        return pltpu.make_async_copy(wuv.at[at], wv.at[at], wv_sem.at[i])

    def w_copy(i, slot):
        rows = pl.ds(pl.multiple_of(core * depth, depth), depth)
        return pltpu.make_async_copy(w_o.at[rows, pl.ds(pl.multiple_of(i * O_BLK, O_BLK), O_BLK)], wbuf.at[slot], w_sem.at[slot])

    def send(i):
        return pltpu.make_async_remote_copy(src_ref=going.at[i], dst_ref=coming.at[i], send_sem=s_send.at[i], recv_sem=s_recv.at[i],
                                            device_id=(partner,), device_id_type=MESH)

    for i in range(n_h):
        for half in range(2):
            lat_copy(half, i).start()
        wv_copy(i).start()
    for i in range(O_BUFS):
        w_copy(i, i).start()

    barrier = pltpu.get_barrier_semaphore()
    pl.semaphore_signal(barrier, inc=1, device_id=(partner,), device_id_type=MESH)
    pl.semaphore_wait(barrier, 1)

    @pl.loop(0, n_h)
    def _(i):
        for half in range(2):
            lat_copy(half, i).wait()
        wv_copy(i).wait()
        for j in range(H_BLK):
            h = i * H_BLK + j
            near = lat[pl.ds(pl.multiple_of(h * CHUNK, CHUNK), CHUNK), :]
            far = lat[pl.ds(pl.multiple_of(HALF + h * CHUNK, CHUNK), CHUNK), :]
            o = jnp.dot(jnp.concatenate([near, far], axis=0), wv[h], preferred_element_type=F32)
            heads[:, pl.ds(pl.multiple_of(h * VALUE_DIM, VALUE_DIM), VALUE_DIM)] = o.astype(BF16)

    @pl.loop(0, n_blk)
    def _(i):
        slot = lax.rem(i, O_BUFS)
        w_copy(i, slot).wait()
        part = jnp.dot(heads[...], wbuf[slot], preferred_element_type=F32)

        @pl.when(i + O_BUFS < n_blk)
        def _():
            w_copy(i + O_BUFS, slot).start()

        own[i] = part[:CHUNK]
        going[i] = part[CHUNK:]

        @pl.when(i > 0)
        def _():
            send(i - 1).start()

    for i in range(n_blk):
        if i == 1:
            send(n_blk - 1).start()
        send(i).wait_recv()
        at = slice(i * O_BLK, (i + 1) * O_BLK)
        y_ref[:, at] = (x_ref[:, at].astype(F32) + (own[i] + coming[i])).astype(BF16)
    for i in range(n_blk):
        send(i).wait_send()


def finish(x, o_lat, wuv, w_o):
    any_spec = pl.BlockSpec(memory_space=pl.ANY)
    vmem = pl.BlockSpec(memory_space=pltpu.VMEM)
    dma = pltpu.SemaphoreType.DMA
    n_h = CORE_HEADS // H_BLK
    n_blk = w_o.shape[1] // O_BLK
    return pl.pallas_call(
        finish_kernel,
        name="finish",
        out_shape=jax.ShapeDtypeStruct(x.shape, BF16),
        in_specs=[vmem] + [any_spec] * 3,
        out_specs=vmem,
        scratch_shapes=[
            pltpu.VMEM(o_lat.shape, BF16),
            pltpu.VMEM(wuv.shape, BF16),
            pltpu.VMEM((2 * CHUNK, CORE_HEADS * VALUE_DIM), BF16),
            pltpu.VMEM((O_BUFS, CORE_HEADS * VALUE_DIM, O_BLK), BF16),
            pltpu.VMEM((n_blk, CHUNK, O_BLK), F32),
            pltpu.VMEM((n_blk, CHUNK, O_BLK), F32),
            pltpu.VMEM((n_blk, CHUNK, O_BLK), F32),
            dma((2, n_h)),
            dma((n_h,)),
            dma((O_BUFS,)),
            dma((n_blk,)),
            dma((n_blk,)),
        ],
        compiler_params=pltpu.CompilerParams(collective_id=1, has_side_effects=True, vmem_limit_bytes=VMEM_LIMIT),
    )(x, o_lat, wuv, w_o)


COPY_PARTS = 8


def cache_kernel(cache_c, cache_kr, page_c, page_k, out_c, out_kr, cbuf, kbuf, in_sem, out_sem):
    pages = cache_c.shape[0] - 1
    step = pages // COPY_PARTS
    ins, outs = [], []
    for i in range(COPY_PARTS):
        at = pl.ds(i * step, step)
        ins.append(pltpu.make_async_copy(cache_c.at[at], cbuf.at[at], in_sem.at[i]))
        outs.append(pltpu.make_async_copy(cbuf.at[at], out_c.at[at], out_sem.at[i]))
    at = pl.ds(0, pages)
    last = pl.ds(pages, 1)
    ins += [pltpu.make_async_copy(cache_kr.at[at], kbuf.at[at], in_sem.at[COPY_PARTS]),
            pltpu.make_async_copy(page_c, cbuf.at[pages], in_sem.at[COPY_PARTS + 1]),
            pltpu.make_async_copy(page_k, kbuf.at[pages], in_sem.at[COPY_PARTS + 2])]
    outs += [pltpu.make_async_copy(kbuf.at[at], out_kr.at[at], out_sem.at[COPY_PARTS]),
             pltpu.make_async_copy(cbuf.at[last], out_c.at[last], out_sem.at[COPY_PARTS + 1]),
             pltpu.make_async_copy(kbuf.at[last], out_kr.at[last], out_sem.at[COPY_PARTS + 2])]
    for c in ins:
        c.start()
    for c, o in zip(ins, outs):
        c.wait()
        o.start()
    for o in outs:
        o.wait()


def update_cache(cache_c, cache_kr, page_c, page_k):
    any_spec = pl.BlockSpec(memory_space=pl.ANY)
    return pl.pallas_call(
        cache_kernel,
        name="cache",
        out_shape=(jax.ShapeDtypeStruct(cache_c.shape, BF16), jax.ShapeDtypeStruct(cache_kr.shape, BF16)),
        in_specs=[any_spec] * 4,
        out_specs=(any_spec, any_spec),
        scratch_shapes=[
            pltpu.VMEM(cache_c.shape, BF16),
            pltpu.VMEM(cache_kr.shape, BF16),
            pltpu.SemaphoreType.DMA((COPY_PARTS + 3,)),
            pltpu.SemaphoreType.DMA((COPY_PARTS + 3,)),
        ],
    )(cache_c, cache_kr, page_c, page_k)


def solution(mesh):
    n = mesh.shape["pool"]

    def device_step(hidden, pre_len, pre_table, wr_table, cache_c, cache_kr, w_q, w_dkv, g_kv, w_uk, w_uv, w_o):
        x = hidden[0]
        me = lax.axis_index("pool")
        owners = pre_table[0, :, 0]
        table_pages = owners.shape[0]
        earlier = jnp.arange(table_pages)[:, None] > jnp.arange(table_pages)[None, :]
        rank = jnp.sum(jnp.where(earlier & (owners[:, None] == owners[None, :]), 1, 0), axis=1)
        pos = jnp.where(owners >= 0, owners * SLOTS + rank, -1)
        lanes = jnp.arange(128, dtype=jnp.int32)
        slot_of = jnp.where(lanes < SLOTS, jnp.arange(n, dtype=jnp.int32)[:, None] * SLOTS + lanes, -2)
        asked = jnp.sum(jnp.where(pos[None, None, :] == slot_of[:, :, None], pre_table[0, :, 1], 0), axis=2)
        ids = jnp.where(lanes == SLOTS, wr_table[0, 0, 0], asked)[:, None, :].astype(jnp.int32)
        keys = jnp.arange(2 * SLOTS * PAGE_LEN, dtype=jnp.int32)
        owner_of = jnp.bitwise_xor(me, jnp.arange(n // 2, dtype=jnp.int32)[:, None] + 16 * (keys // (SLOTS * PAGE_LEN)))
        counts = jnp.sum(jnp.where(owner_of[:, :: SLOTS * PAGE_LEN, None] == owners, 1, 0), axis=2)
        counts = jnp.repeat(counts, SLOTS * PAGE_LEN, axis=1)
        bias = jnp.where((keys // PAGE_LEN) % SLOTS < counts, 0.0, -jnp.inf).astype(F32)[:, None, :]
        cos_tab, sin_tab = rope_tables(pre_len[0] + jnp.arange(CHUNK))
        rot = jnp.stack([jnp.concatenate([cos_tab, cos_tab], -1), jnp.concatenate([-sin_tab, sin_tab], -1)])
        o_lat, wuv, page_c, page_k = layer(n, ids, bias, rot, g_kv.astype(F32)[None], x, cache_c[0], cache_kr[0], w_q, w_dkv.T, w_uk, w_uv)
        y = finish(x, o_lat, wuv, w_o)
        out_c, out_kr = update_cache(cache_c[0], cache_kr[0], page_c, page_k)
        return y[None], out_c[None], out_kr[None]

    row_spec = P("pool")
    rep_spec = P()
    return jax.shard_map(device_step, mesh=mesh, in_specs=(row_spec,) * 6 + (rep_spec,) * 6, out_specs=(row_spec,) * 3, check_vma=False)


def rope_tables(positions):
    half_dim = ROPE_DIM // 2
    inv_freq = ROPE_BASE ** (-jnp.arange(half_dim, dtype=F32) / half_dim)
    angles = positions.astype(F32)[..., None] * inv_freq
    return jnp.cos(angles), jnp.sin(angles)
```

```python
import functools

import jax
import jax.numpy as jnp
from jax import lax
from jax.experimental import pallas as pl
from jax.experimental.pallas import tpu as pltpu
from jax.sharding import PartitionSpec as P

PAGE_LEN = 64
LATENT = 512
ROPE_DIM = 64
NOPE_DIM = 128
VALUE_DIM = 128
HEADS = 64
CHUNK = 64
D_MODEL = 7168
SLOTS = 4
NORM_EPS = 1e-6
ROPE_BASE = 10000.0
MESH = pl.DeviceIdType.MESH
VMEM_LIMIT = 63 * 1024 * 1024
SCALE2 = (NOPE_DIM + ROPE_DIM) ** -0.5 * 1.4426950408889634
ROWS = HEADS * CHUNK
SUB = 256
SUBS = 4
W_BLK = 512
W_ROWS = 1792
W_BUFS = 4
KV_ROWS = 512
H_BLK = 8
CORE_HEADS = HEADS // 2
HALF = CORE_HEADS * CHUNK
RING = 3
LAST_DIMS = (((1,), (1,)), ((), ()))
BF16 = jnp.bfloat16
F32 = jnp.float32


def step_code(k):
    i, q = lax.div(k, 4), lax.rem(k, 4)
    return i + 8 * (2 * lax.rem(lax.div(q + 1, 2), 2) + lax.div(q, 2))


def flip_weights(me, bits):
    return [2 ** i - 2 ** (i + 1) * lax.rem(lax.div(me, 2 ** i), 2) for i in range(bits)]


def flipped(me, flips, code):
    out = me
    for i, f in enumerate(flips):
        out = out + f * lax.rem(lax.div(code, 2 ** i), 2)
    return out


def rope(values, cos2, sin2):
    half = ROPE_DIM // 2
    swapped = jnp.concatenate([values[:, half:], values[:, :half]], axis=-1)
    return values * cos2 + swapped * sin2


def layer_kernel(n, ids_ref, bias_ref, rot_ref, gain_ref, x_ref, cache_c, cache_kr, w_q, w_dkv, w_uk, w_uv,
                 o_lat, wuv_out, page_c_out, page_k_out,
                 ids_in, ids_smem, cc, ck, kp, stage_c, stage_k, land_c, land_k, ring_c, ring_k, wbuf, q_all, qc, qk, m_ref, l_ref, acc,
                 hbuf, h32, hout, kvbuf, xb, bias_p, rot_p, new_c, new_k, kk, part_out, part_mid, part_fwd, part_in, c32,
                 loc_sem, id_send, id_recv, c_send, c_recv, k_send, k_recv, p_send, p_recv, f_send, f_recv, w_sem, h_sem, ho_sem, kv_sem, out_sem,
                 pair_send, pair_recv, rc_send, rc_recv, rk_send, rk_recv, credit):
    me = lax.axis_index("pool")
    bits = n.bit_length() - 1
    pages = kp.shape[0]
    core = lax.rem(me, 2)
    n_blk = w_q.shape[1] // 2 // W_BLK
    n_kv = D_MODEL // KV_ROWS
    n_h = CORE_HEADS // H_BLK

    load_c = pltpu.make_async_copy(cache_c.at[pl.ds(0, pages)], cc, loc_sem.at[0])
    load_k = pltpu.make_async_copy(cache_kr.at[pl.ds(0, pages)], ck, loc_sem.at[1])
    load_k.start()
    load_c.start()

    flips = flip_weights(me, bits)
    any_peer = lax.rem(me + 1, n)
    partner = me + flips[0]

    def peer_of(k):
        return flipped(me, flips, step_code(k))

    barrier = pltpu.get_barrier_semaphore()

    @pl.loop(1, n)
    def _(k):
        pl.semaphore_signal(barrier, inc=1, device_id=(peer_of(k),), device_id_type=MESH)

    def kv_copy(i, slot):
        return pltpu.make_async_copy(w_dkv.at[:, pl.ds(i * KV_ROWS, KV_ROWS)], kvbuf.at[slot], kv_sem.at[slot])

    n_row = D_MODEL // W_ROWS

    def w_copy(col, r):
        rows = pl.ds(r * W_ROWS, W_ROWS)
        return pltpu.make_async_copy(w_q.at[rows, pl.ds(pl.multiple_of((core * n_blk + col) * W_BLK, W_BLK), W_BLK)], wbuf.at[r], w_sem.at[r])

    kv_copy(0, 0).start()
    kv_copy(1, 1).start()
    own_x = pltpu.make_async_copy(x_ref, xb.at[pl.ds(0, CHUNK)], loc_sem.at[4])
    own_x.start()
    pl.semaphore_wait(barrier, n - 1)

    def pair_copy(i, src, dst):
        return pltpu.make_async_remote_copy(src_ref=src, dst_ref=dst, send_sem=pair_send.at[i], recv_sem=pair_recv.at[i],
                                            device_id=(partner,), device_id_type=MESH)

    pair = [pair_copy(0, x_ref, xb.at[pl.ds(CHUNK, CHUNK)]), pair_copy(1, rot_ref, rot_p), pair_copy(2, bias_ref, bias_p)]

    def id_copy(k, peer):
        return pltpu.make_async_remote_copy(src_ref=ids_ref.at[peer], dst_ref=ids_in.at[k], send_sem=id_send.at[k],
                                            recv_sem=id_recv.at[k], device_id=(peer,), device_id_type=MESH)

    @pl.loop(1, n)
    def _(k):
        id_copy(k, peer_of(k)).start()

    own_ids = pltpu.make_async_copy(ids_ref.at[me], ids_in.at[0], loc_sem.at[2])
    own_ids.start()
    for c in pair:
        c.start()
    load_k.wait()

    @pl.loop(0, pages)
    def _(i):
        page = ck[i]
        kp[i] = jnp.concatenate([page[: PAGE_LEN // 2], page[PAGE_LEN // 2:]], axis=-1)

    load_c.wait()
    own_ids.wait()

    @pl.loop(1, n)
    def _(k):
        id_copy(k, any_peer).wait_recv()

    to_smem = pltpu.make_async_copy(ids_in, ids_smem, loc_sem.at[3])
    to_smem.start()
    to_smem.wait()

    def c_copy(k, peer):
        return pltpu.make_async_remote_copy(src_ref=stage_c.at[k], dst_ref=land_c.at[k], send_sem=c_send.at[k],
                                            recv_sem=c_recv.at[k], device_id=(peer,), device_id_type=MESH)

    def k_copy(k, peer):
        return pltpu.make_async_remote_copy(src_ref=stage_k.at[k], dst_ref=land_k.at[k], send_sem=k_send.at[k],
                                            recv_sem=k_recv.at[k], device_id=(peer,), device_id_type=MESH)

    def launch(k):
        peer = peer_of(k)
        c_copy(k, peer).start()
        k_copy(k, peer).start()

    def send_pages(k, first):
        for s in range(SLOTS):
            page = ids_smem[k, 0, s]
            stage_c[k, s] = cc[page]
            stage_k[k, s] = kp[page]

        @pl.when(k > first)
        def _():
            launch(k - 1)

    @pl.loop(1, n // 2)
    def _(k):
        send_pages(k, 1)

    launch(n // 2 - 1)

    for r in range(n_row):
        w_copy(0, r).start()

    own_x.wait()
    for c in pair:
        c.wait_recv()
    kv = jnp.zeros((2 * CHUNK, LATENT + ROPE_DIM), F32)
    for i in range(n_kv):
        kv_copy(i, i % 2).wait()
        kv = kv + lax.dot_general(xb[:, i * KV_ROWS:(i + 1) * KV_ROWS], kvbuf[i % 2], LAST_DIMS, preferred_element_type=F32)
        if i + 2 < n_kv:
            kv_copy(i + 2, i % 2).start()
    lat = kv[:, :LATENT]
    inv_rms = lax.rsqrt(jnp.mean(lat * lat, axis=-1, keepdims=True) + NORM_EPS)
    c_new = (lat * inv_rms * gain_ref[...]).astype(BF16)
    cos2 = jnp.concatenate([rot_ref[0], rot_p[0]], axis=0)
    sin2 = jnp.concatenate([rot_ref[1], rot_p[1]], axis=0)
    kr_new = rope(kv[:, LATENT:], cos2, sin2).astype(BF16)
    new_c[...] = c_new
    new_k[...] = kr_new

    for g in range(LATENT // 128):
        c32[:, g, :] = c_new[:CHUNK, g * 128:(g + 1) * 128].astype(F32)
    c32[:, 4, :] = jnp.concatenate([kr_new[:CHUNK], kr_new[:CHUNK]], axis=-1).astype(F32)
    low = lax.broadcasted_iota(jnp.int32, (1, 128), 1) < ROPE_DIM
    for i in range(n):
        a = c32[2 * i]
        b = c32[2 * i + 1]
        last = jnp.where(low, a[4:5], b[4:5])
        part_out[i] = jnp.concatenate([a[:4], b[:4], jnp.broadcast_to(last, (8, 128))], axis=0).astype(BF16)

    def p_copy(k, peer):
        return pltpu.make_async_remote_copy(src_ref=part_out.at[peer], dst_ref=part_mid.at[k], send_sem=p_send.at[k],
                                            recv_sem=p_recv.at[k], device_id=(peer,), device_id_type=MESH)

    def f_copy(k, peer):
        return pltpu.make_async_remote_copy(src_ref=part_fwd.at[k], dst_ref=part_in.at[me], send_sem=f_send.at[k],
                                            recv_sem=f_recv.at[k], device_id=(peer,), device_id_type=MESH)

    @pl.loop(1, n)
    def _(k):
        p_copy(k, peer_of(k)).start()

    part_mid[0] = part_out[me]

    @pl.loop(n // 2, n)
    def _(k):
        send_pages(k, n // 2)

    for s in range(SLOTS):
        page = ids_smem[0, 0, s]
        land_c[0, s] = cc[page]
        land_k[0, s] = kp[page]
    launch(n - 1)

    @pl.loop(0, n_blk)
    def _(col):
        total = jnp.zeros((2 * CHUNK, W_BLK), F32)
        for r in range(n_row):
            w_copy(col, r).wait()
            total = total + jnp.dot(xb[:, r * W_ROWS:(r + 1) * W_ROWS], wbuf[r], preferred_element_type=F32)

            @pl.when(col + 1 < n_blk)
            def _():
                w_copy(col + 1, r).start()

        q_all[:, pl.ds(pl.multiple_of(col * W_BLK, W_BLK), W_BLK)] = total.astype(BF16)

    def h_copy(src, i, slot):
        return pltpu.make_async_copy(src.at[:, pl.ds(pl.multiple_of(core * CORE_HEADS + i * H_BLK, H_BLK), H_BLK)], hbuf.at[slot], h_sem.at[slot])

    h_copy(w_uk, 0, 0).start()

    @pl.loop(0, n_h)
    def _(i):
        slot = i % 2
        h_copy(w_uk, i, slot).wait()

        @pl.when(i + 1 < n_h)
        def _():
            h_copy(w_uk, i + 1, 1 - slot).start()

        h32[...] = hbuf[slot].astype(F32)
        for pair in range(H_BLK // 2):
            q2 = q_all[:, pl.ds(pl.multiple_of((i * (H_BLK // 2) + pair) * 384, 128), 384)]
            q32 = q2.astype(F32)
            for odd in range(2):
                j = pair * 2 + odd
                base = odd * (NOPE_DIM + ROPE_DIM)
                wk = h32[:, j, :].astype(BF16)
                u = lax.dot_general(q2[:, base:base + NOPE_DIM], wk, LAST_DIMS, preferred_element_type=F32)
                qr = rope(q32[:, base + NOPE_DIM:base + NOPE_DIM + ROPE_DIM], cos2, sin2).astype(BF16)
                at = pl.ds(pl.multiple_of((i * H_BLK + j) * CHUNK, CHUNK), CHUNK)
                far = pl.ds(pl.multiple_of((CORE_HEADS + i * H_BLK + j) * CHUNK, CHUNK), CHUNK)
                qc[at, :] = u[:CHUNK].astype(BF16)
                qc[far, :] = u[CHUNK:].astype(BF16)
                twice = jnp.concatenate([qr, qr], axis=-1)
                qk[at, :] = twice[:CHUNK]
                qk[far, :] = twice[CHUNK:]

    def ho_copy(i):
        return pltpu.make_async_copy(hout, wuv_out.at[pl.ds(pl.multiple_of(i * H_BLK, H_BLK), H_BLK)], ho_sem.at[0])

    h_copy(w_uv, 0, 0).start()

    @pl.loop(0, n_h)
    def _(i):
        slot = i % 2
        h_copy(w_uv, i, slot).wait()

        @pl.when(i + 1 < n_h)
        def _():
            h_copy(w_uv, i + 1, 1 - slot).start()

        h32[...] = hbuf[slot].astype(F32)

        @pl.when(i > 0)
        def _():
            ho_copy(i - 1).wait()

        for j in range(H_BLK):
            hout[j] = h32[:, j, :].astype(BF16)
        ho_copy(i).start()

    def tile(at, s, keys):
        m_old = m_ref[at, :]
        m_new = jnp.maximum(m_old, jnp.max(s, axis=-1, keepdims=True))
        alpha = jnp.exp2(m_old - m_new)
        groups = s.shape[1] // 128
        parts = [jnp.exp2(s[:, g * 128:(g + 1) * 128] - m_new) for g in range(groups)]
        total = parts[0]
        for p in parts[1:]:
            total = total + p
        m_ref[at, :] = m_new
        l_ref[at, :] = l_ref[at, :] * alpha + total
        p = jnp.concatenate([p.astype(BF16) for p in parts], axis=-1)
        pv = jnp.dot(p, keys, preferred_element_type=F32)
        for g in range(LATENT // 128):
            lanes = slice(g * 128, (g + 1) * 128)
            acc[at, lanes] = acc[at, lanes] * alpha + pv[:, lanes]

    def row_tiles(half, i):
        return [pl.ds(pl.multiple_of(half * HALF + (i * SUBS + u) * SUB, SUB), SUB) for u in range(SUBS)]

    for half in range(2):
        @pl.loop(0, HALF // (SUB * SUBS))
        def _(i):
            causal = (lax.broadcasted_iota(jnp.int32, (SUB, CHUNK), 1) <= lax.broadcasted_iota(jnp.int32, (SUB, CHUNK), 0) % CHUNK)
            c64 = new_c[half * CHUNK:(half + 1) * CHUNK, :]
            k64 = jnp.concatenate([new_k[half * CHUNK:(half + 1) * CHUNK, :], jnp.zeros((CHUNK, ROPE_DIM), BF16)], axis=-1)
            ats = row_tiles(half, i)
            raw = []
            for at in ats:
                s = lax.dot_general(qc[at, :], c64, LAST_DIMS, preferred_element_type=F32)
                raw.append(s + lax.dot_general(qk[at, :], k64, LAST_DIMS, preferred_element_type=F32))
            for at, s in zip(ats, raw):
                s = jnp.where(causal, s * SCALE2, -jnp.inf)
                m = jnp.max(s, axis=-1, keepdims=True)
                p = jnp.exp2(s - m)
                m_ref[at, :] = jnp.broadcast_to(m, (SUB, 128))
                l_ref[at, :] = jnp.concatenate([p, jnp.zeros((SUB, 128 - CHUNK), F32)], axis=-1)
                acc[at, :] = jnp.dot(p.astype(BF16), c64, preferred_element_type=F32)

    half_low = lax.broadcasted_iota(jnp.int32, (PAGE_LEN // 2, 2 * ROPE_DIM), 1) < ROPE_DIM

    def spread(page_of):
        for d in range(2):
            for s in range(SLOTS):
                page = page_of(d, s)
                zero = jnp.zeros_like(page)
                base = (d * SLOTS + s) * PAGE_LEN
                kk[base:base + PAGE_LEN // 2, :] = jnp.where(half_low, page, zero)
                kk[base + PAGE_LEN // 2:base + PAGE_LEN, :] = jnp.where(half_low, zero, page)

    def attend(half, keys_of, bias_of):
        @pl.loop(0, HALF // (SUB * SUBS))
        def _(i):
            keys = keys_of().reshape(2 * SLOTS * PAGE_LEN, LATENT)
            bias = bias_of()
            ats = row_tiles(half, i)
            raw = []
            for at in ats:
                s = lax.dot_general(qc[at, :], keys, LAST_DIMS, preferred_element_type=F32)
                raw.append(s + lax.dot_general(qk[at, :], kk[...], LAST_DIMS, preferred_element_type=F32))
            for at, s in zip(ats, raw):
                tile(at, s * SCALE2 + bias, keys)

    steps = n // 2

    def ring_copies(t):
        r = lax.rem(t, RING)
        return (pltpu.make_async_remote_copy(src_ref=land_c.at[pl.ds(2 * t, 2)], dst_ref=ring_c.at[r], send_sem=rc_send.at[r],
                                             recv_sem=rc_recv.at[r], device_id=(partner,), device_id_type=MESH),
                pltpu.make_async_remote_copy(src_ref=land_k.at[pl.ds(2 * t, 2)], dst_ref=ring_k.at[r], send_sem=rk_send.at[r],
                                             recv_sem=rk_recv.at[r], device_id=(partner,), device_id_type=MESH))

    @pl.loop(0, steps + 1)
    def _(t):
        @pl.when(t < steps)
        def _():
            @pl.when(t > 0)
            def _():
                c_copy(2 * t, any_peer).wait_recv()
                k_copy(2 * t, any_peer).wait_recv()

            c_copy(2 * t + 1, any_peer).wait_recv()
            k_copy(2 * t + 1, any_peer).wait_recv()

            @pl.when(t >= RING)
            def _():
                for c in ring_copies(t - RING):
                    c.wait_send()
                pl.semaphore_wait(credit, 1)

            for c in ring_copies(t):
                c.start()
            spread(lambda d, s: land_k[2 * t + d, s])
            attend(0, lambda: land_c[pl.ds(2 * t, 2)], lambda: bias_ref[t])

        @pl.when(t > 0)
        def _():
            r = lax.rem(t - 1, RING)
            for c in ring_copies(t - 1):
                c.wait_recv()
            spread(lambda d, s: ring_k[r, d, s])
            attend(1, lambda: ring_c[r], lambda: bias_p[t - 1])

            @pl.when(t - 1 < steps - RING)
            def _():
                pl.semaphore_signal(credit, inc=1, device_id=(partner,), device_id_type=MESH)

        @pl.when(t == n // 2 - 6)
        def _():
            @pl.loop(1, n)
            def _(k):
                p_copy(k, any_peer).wait_recv()

            @pl.loop(0, n)
            def _(k):
                owner = peer_of(k)
                source = jnp.int32(0)
                for j in range(n):
                    source = jnp.where(ids_smem[j, 0, SLOTS] == owner, j, source)
                part_fwd[k] = part_mid[source]

            @pl.loop(1, n)
            def _(k):
                f_copy(k, peer_of(k)).start()

            part_in[me] = part_fwd[0]

    @pl.loop(0, ROWS // SUB)
    def _(i):
        at = pl.ds(pl.multiple_of(i * SUB, SUB), SUB)
        share = 1.0 / jnp.sum(l_ref[at, :], axis=-1, keepdims=True)
        qc[at, :] = (acc[at, :] * share).astype(BF16)

    out = pltpu.make_async_copy(qc, o_lat, out_sem.at[0])
    out.start()

    @pl.loop(1, n)
    def _(k):
        f_copy(k, any_peer).wait_recv()

    for i in range(n):
        part = part_in[i].astype(F32)
        c32[2 * i, 0:4] = part[0:4]
        c32[2 * i + 1, 0:4] = part[4:8]
        c32[2 * i, 4:5] = part[8:9]
        c32[2 * i + 1, 4:5] = jnp.concatenate([part[8:9, ROPE_DIM:], part[8:9, :ROPE_DIM]], axis=-1)
    for g in range(LATENT // 128):
        new_c[:CHUNK, g * 128:(g + 1) * 128] = c32[:, g, :].astype(BF16)
    new_k[:CHUNK, :] = c32[:, 4, :][:, :ROPE_DIM].astype(BF16)
    out_pc = pltpu.make_async_copy(new_c.at[pl.ds(0, CHUNK)], page_c_out, out_sem.at[1])
    out_pk = pltpu.make_async_copy(new_k.at[pl.ds(0, CHUNK)], page_k_out, out_sem.at[2])
    out_pc.start()
    out_pk.start()

    @pl.loop(1, n)
    def _(k):
        id_copy(k, any_peer).wait_send()
        c_copy(k, any_peer).wait_send()
        k_copy(k, any_peer).wait_send()
        p_copy(k, any_peer).wait_send()
        f_copy(k, any_peer).wait_send()

    for c in pair:
        c.wait_send()
    for t in range(steps - RING, steps):
        for c in ring_copies(t):
            c.wait_send()
    ho_copy(n_h - 1).wait()
    out.wait()
    out_pc.wait()
    out_pk.wait()


def layer(n, ids, bias, rot, gain, x, cache_c, cache_kr, w_q, w_dkv, w_uk, w_uv):
    pages = cache_c.shape[0] - 1
    any_spec = pl.BlockSpec(memory_space=pl.ANY)
    vmem = pl.BlockSpec(memory_space=pltpu.VMEM)
    dma = pltpu.SemaphoreType.DMA
    return pl.pallas_call(
        functools.partial(layer_kernel, n),
        name="layer",
        out_shape=(
            jax.ShapeDtypeStruct((ROWS, LATENT), BF16),
            jax.ShapeDtypeStruct((CORE_HEADS, LATENT, VALUE_DIM), BF16),
            jax.ShapeDtypeStruct((CHUNK, LATENT), BF16),
            jax.ShapeDtypeStruct((CHUNK, ROPE_DIM), BF16),
        ),
        in_specs=[vmem] * 4 + [any_spec] * 7,
        out_specs=(any_spec,) * 4,
        scratch_shapes=[
            pltpu.VMEM((n, 1, 128), jnp.int32),
            pltpu.SMEM((n, 1, 128), jnp.int32),
            pltpu.VMEM((pages, PAGE_LEN, LATENT), BF16),
            pltpu.VMEM((pages, PAGE_LEN, ROPE_DIM), BF16),
            pltpu.VMEM((pages, PAGE_LEN // 2, 2 * ROPE_DIM), BF16),
            pltpu.VMEM((n, SLOTS, PAGE_LEN, LATENT), BF16),
            pltpu.VMEM((n, SLOTS, PAGE_LEN // 2, 2 * ROPE_DIM), BF16),
            pltpu.VMEM((n, SLOTS, PAGE_LEN, LATENT), BF16),
            pltpu.VMEM((n, SLOTS, PAGE_LEN // 2, 2 * ROPE_DIM), BF16),
            pltpu.VMEM((RING, 2, SLOTS, PAGE_LEN, LATENT), BF16),
            pltpu.VMEM((RING, 2, SLOTS, PAGE_LEN // 2, 2 * ROPE_DIM), BF16),
            pltpu.VMEM((W_BUFS, W_ROWS, W_BLK), BF16),
            pltpu.VMEM((2 * CHUNK, CORE_HEADS * (NOPE_DIM + ROPE_DIM)), BF16),
            pltpu.VMEM((ROWS, LATENT), BF16),
            pltpu.VMEM((ROWS, 2 * ROPE_DIM), BF16),
            pltpu.VMEM((ROWS, 128), F32),
            pltpu.VMEM((ROWS, 128), F32),
            pltpu.VMEM((ROWS, LATENT), F32),
            pltpu.VMEM((2, LATENT, H_BLK, NOPE_DIM), BF16),
            pltpu.VMEM((LATENT, H_BLK, NOPE_DIM), F32),
            pltpu.VMEM((H_BLK, LATENT, VALUE_DIM), BF16),
            pltpu.VMEM((2, LATENT + ROPE_DIM, KV_ROWS), BF16),
            pltpu.VMEM((2 * CHUNK, D_MODEL), BF16),
            pltpu.VMEM(bias.shape, F32),
            pltpu.VMEM(rot.shape, F32),
            pltpu.VMEM((2 * CHUNK, LATENT), BF16),
            pltpu.VMEM((2 * CHUNK, ROPE_DIM), BF16),
            pltpu.VMEM((2 * SLOTS * PAGE_LEN, 2 * ROPE_DIM), BF16),
            pltpu.VMEM((n, 16, 128), BF16),
            pltpu.VMEM((n, 16, 128), BF16),
            pltpu.VMEM((n, 16, 128), BF16),
            pltpu.VMEM((n, 16, 128), BF16),
            pltpu.VMEM((CHUNK, 8, 128), F32),
            dma((5,)),
        ] + [dma((n,))] * 10 + [dma((W_BUFS,)), dma((2,)), dma((1,)), dma((2,)), dma((3,)), dma((3,)), dma((3,))] + [dma((RING,))] * 4 + [pltpu.SemaphoreType.REGULAR],
        compiler_params=pltpu.CompilerParams(collective_id=0, has_side_effects=True, vmem_limit_bytes=VMEM_LIMIT),
    )(ids, bias, rot, gain, x, cache_c, cache_kr, w_q, w_dkv, w_uk, w_uv)


O_BLK = 512
O_BUFS = 7


def finish_kernel(x_ref, o_lat, wuv, w_o, y_ref, lat, wv, heads, wbuf, own, going, coming, lat_sem, wv_sem, w_sem, s_send, s_recv):
    me = lax.axis_index("pool")
    core = lax.rem(me, 2)
    partner = me + 1 - 2 * core
    depth = CORE_HEADS * VALUE_DIM
    n_blk = w_o.shape[1] // O_BLK
    n_h = CORE_HEADS // H_BLK

    def lat_copy(half, i):
        at = pl.ds(pl.multiple_of(half * HALF + i * H_BLK * CHUNK, 8), H_BLK * CHUNK)
        return pltpu.make_async_copy(o_lat.at[at], lat.at[at], lat_sem.at[half, i])

    def wv_copy(i):
        at = pl.ds(pl.multiple_of(i * H_BLK, H_BLK), H_BLK)
        return pltpu.make_async_copy(wuv.at[at], wv.at[at], wv_sem.at[i])

    def w_copy(i, slot):
        rows = pl.ds(pl.multiple_of(core * depth, depth), depth)
        return pltpu.make_async_copy(w_o.at[rows, pl.ds(pl.multiple_of(i * O_BLK, O_BLK), O_BLK)], wbuf.at[slot], w_sem.at[slot])

    def send(i):
        return pltpu.make_async_remote_copy(src_ref=going.at[i], dst_ref=coming.at[i], send_sem=s_send.at[i], recv_sem=s_recv.at[i],
                                            device_id=(partner,), device_id_type=MESH)

    for i in range(n_h):
        for half in range(2):
            lat_copy(half, i).start()
        wv_copy(i).start()
    for i in range(O_BUFS):
        w_copy(i, i).start()

    barrier = pltpu.get_barrier_semaphore()
    pl.semaphore_signal(barrier, inc=1, device_id=(partner,), device_id_type=MESH)
    pl.semaphore_wait(barrier, 1)

    @pl.loop(0, n_h)
    def _(i):
        for half in range(2):
            lat_copy(half, i).wait()
        wv_copy(i).wait()
        for j in range(H_BLK):
            h = i * H_BLK + j
            near = lat[pl.ds(pl.multiple_of(h * CHUNK, CHUNK), CHUNK), :]
            far = lat[pl.ds(pl.multiple_of(HALF + h * CHUNK, CHUNK), CHUNK), :]
            o = jnp.dot(jnp.concatenate([near, far], axis=0), wv[h], preferred_element_type=F32)
            heads[:, pl.ds(pl.multiple_of(h * VALUE_DIM, VALUE_DIM), VALUE_DIM)] = o.astype(BF16)

    @pl.loop(0, n_blk)
    def _(i):
        slot = lax.rem(i, O_BUFS)
        w_copy(i, slot).wait()
        part = jnp.dot(heads[...], wbuf[slot], preferred_element_type=F32)

        @pl.when(i + O_BUFS < n_blk)
        def _():
            w_copy(i + O_BUFS, slot).start()

        own[i] = part[:CHUNK]
        going[i] = part[CHUNK:]

        @pl.when(i > 0)
        def _():
            send(i - 1).start()

    for i in range(n_blk):
        if i == 1:
            send(n_blk - 1).start()
        send(i).wait_recv()
        at = slice(i * O_BLK, (i + 1) * O_BLK)
        y_ref[:, at] = (x_ref[:, at].astype(F32) + (own[i] + coming[i])).astype(BF16)
    for i in range(n_blk):
        send(i).wait_send()


def finish(x, o_lat, wuv, w_o):
    any_spec = pl.BlockSpec(memory_space=pl.ANY)
    vmem = pl.BlockSpec(memory_space=pltpu.VMEM)
    dma = pltpu.SemaphoreType.DMA
    n_h = CORE_HEADS // H_BLK
    n_blk = w_o.shape[1] // O_BLK
    return pl.pallas_call(
        finish_kernel,
        name="finish",
        out_shape=jax.ShapeDtypeStruct(x.shape, BF16),
        in_specs=[vmem] + [any_spec] * 3,
        out_specs=vmem,
        scratch_shapes=[
            pltpu.VMEM(o_lat.shape, BF16),
            pltpu.VMEM(wuv.shape, BF16),
            pltpu.VMEM((2 * CHUNK, CORE_HEADS * VALUE_DIM), BF16),
            pltpu.VMEM((O_BUFS, CORE_HEADS * VALUE_DIM, O_BLK), BF16),
            pltpu.VMEM((n_blk, CHUNK, O_BLK), F32),
            pltpu.VMEM((n_blk, CHUNK, O_BLK), F32),
            pltpu.VMEM((n_blk, CHUNK, O_BLK), F32),
            dma((2, n_h)),
            dma((n_h,)),
            dma((O_BUFS,)),
            dma((n_blk,)),
            dma((n_blk,)),
        ],
        compiler_params=pltpu.CompilerParams(collective_id=1, has_side_effects=True, vmem_limit_bytes=VMEM_LIMIT),
    )(x, o_lat, wuv, w_o)


COPY_PARTS = 8


def cache_kernel(cache_c, cache_kr, page_c, page_k, out_c, out_kr, cbuf, kbuf, in_sem, out_sem):
    pages = cache_c.shape[0] - 1
    step = pages // COPY_PARTS
    ins, outs = [], []
    for i in range(COPY_PARTS):
        at = pl.ds(i * step, step)
        ins.append(pltpu.make_async_copy(cache_c.at[at], cbuf.at[at], in_sem.at[i]))
        outs.append(pltpu.make_async_copy(cbuf.at[at], out_c.at[at], out_sem.at[i]))
    at = pl.ds(0, pages)
    last = pl.ds(pages, 1)
    ins += [pltpu.make_async_copy(cache_kr.at[at], kbuf.at[at], in_sem.at[COPY_PARTS]),
            pltpu.make_async_copy(page_c, cbuf.at[pages], in_sem.at[COPY_PARTS + 1]),
            pltpu.make_async_copy(page_k, kbuf.at[pages], in_sem.at[COPY_PARTS + 2])]
    outs += [pltpu.make_async_copy(kbuf.at[at], out_kr.at[at], out_sem.at[COPY_PARTS]),
             pltpu.make_async_copy(cbuf.at[last], out_c.at[last], out_sem.at[COPY_PARTS + 1]),
             pltpu.make_async_copy(kbuf.at[last], out_kr.at[last], out_sem.at[COPY_PARTS + 2])]
    for c in ins:
        c.start()
    for c, o in zip(ins, outs):
        c.wait()
        o.start()
    for o in outs:
        o.wait()


def update_cache(cache_c, cache_kr, page_c, page_k):
    any_spec = pl.BlockSpec(memory_space=pl.ANY)
    return pl.pallas_call(
        cache_kernel,
        name="cache",
        out_shape=(jax.ShapeDtypeStruct(cache_c.shape, BF16), jax.ShapeDtypeStruct(cache_kr.shape, BF16)),
        in_specs=[any_spec] * 4,
        out_specs=(any_spec, any_spec),
        scratch_shapes=[
            pltpu.VMEM(cache_c.shape, BF16),
            pltpu.VMEM(cache_kr.shape, BF16),
            pltpu.SemaphoreType.DMA((COPY_PARTS + 3,)),
            pltpu.SemaphoreType.DMA((COPY_PARTS + 3,)),
        ],
    )(cache_c, cache_kr, page_c, page_k)


def solution(mesh):
    n = mesh.shape["pool"]

    def device_step(hidden, pre_len, pre_table, wr_table, cache_c, cache_kr, w_q, w_dkv, g_kv, w_uk, w_uv, w_o):
        x = hidden[0]
        me = lax.axis_index("pool")
        owners = pre_table[0, :, 0]
        table_pages = owners.shape[0]
        earlier = jnp.arange(table_pages)[:, None] > jnp.arange(table_pages)[None, :]
        rank = jnp.sum(jnp.where(earlier & (owners[:, None] == owners[None, :]), 1, 0), axis=1)
        pos = jnp.where(owners >= 0, owners * SLOTS + rank, -1)
        lanes = jnp.arange(128, dtype=jnp.int32)
        slot_of = jnp.where(lanes < SLOTS, jnp.arange(n, dtype=jnp.int32)[:, None] * SLOTS + lanes, -2)
        asked = jnp.sum(jnp.where(pos[None, None, :] == slot_of[:, :, None], pre_table[0, :, 1], 0), axis=2)
        ids = jnp.where(lanes == SLOTS, wr_table[0, 0, 0], asked)[:, None, :].astype(jnp.int32)
        keys = jnp.arange(2 * SLOTS * PAGE_LEN, dtype=jnp.int32)
        codes = step_code(2 * jnp.arange(n // 2, dtype=jnp.int32)[:, None] + keys // (SLOTS * PAGE_LEN))
        owner_of = jnp.bitwise_xor(me, codes)
        counts = jnp.sum(jnp.where(owner_of[:, :: SLOTS * PAGE_LEN, None] == owners, 1, 0), axis=2)
        counts = jnp.repeat(counts, SLOTS * PAGE_LEN, axis=1)
        bias = jnp.where((keys // PAGE_LEN) % SLOTS < counts, 0.0, -jnp.inf).astype(F32)[:, None, :]
        cos_tab, sin_tab = rope_tables(pre_len[0] + jnp.arange(CHUNK))
        rot = jnp.stack([jnp.concatenate([cos_tab, cos_tab], -1), jnp.concatenate([-sin_tab, sin_tab], -1)])
        o_lat, wuv, page_c, page_k = layer(n, ids, bias, rot, g_kv.astype(F32)[None], x, cache_c[0], cache_kr[0], w_q, w_dkv.T, w_uk, w_uv)
        y = finish(x, o_lat, wuv, w_o)
        out_c, out_kr = update_cache(cache_c[0], cache_kr[0], page_c, page_k)
        return y[None], out_c[None], out_kr[None]

    row_spec = P("pool")
    rep_spec = P()
    return jax.shard_map(device_step, mesh=mesh, in_specs=(row_spec,) * 6 + (rep_spec,) * 6, out_specs=(row_spec,) * 3, check_vma=False)


def rope_tables(positions):
    half_dim = ROPE_DIM // 2
    inv_freq = ROPE_BASE ** (-jnp.arange(half_dim, dtype=F32) / half_dim)
    angles = positions.astype(F32)[..., None] * inv_freq
    return jnp.cos(angles), jnp.sin(angles)
```
